32 devices in a mesh: row: 4 (over y, x), col: 8 (over z, core).
Axes of the slice: x: 2, y: 2, z: 4, core: 2. Of those that a mesh axis runs over, the one named last changes fastest.
Arguments:
- pair_rep: bfloat16 [256, 256, 128], P('row', 'col'), may hold values from -6 to 6
- proj_weight: bfloat16 [2, 4, 128, 128], replicated, may hold values from -0.5 to 0.5
- gate_weight: bfloat16 [2, 128, 128], replicated, may hold values from -0.5 to 0.5
- out_weight: bfloat16 [2, 128, 128], replicated, may hold values from -0.5 to 0.5
- in_gain: float32 [2, 128], replicated, may hold values from 0.1 to 1.9
- out_gain: float32 [2, 128], replicated, may hold values from 0.1 to 1.9
Outputs:
- updated_pair: bfloat16 [256, 256, 128], P('row', 'col')
The draws below stay inside these ranges and needn't reach their ends.
All inputs are finite; a program needn't handle non-finite values.
Results may differ from the reference program's by a relative error of at most 0.011.
Values may be sent and summed in bfloat16 or wider, within the bound.
A program may use at most 64 MiB of HBM per device.

```python
import math
import jax
import jax.numpy as jnp
from jax import lax

C = 128
H = 128
N = 256


def steps_of(own_key, extent, cuts, smallest, largest):
    def one(position, parts):
        draws = jax.random.uniform(jax.random.fold_in(jax.random.fold_in(own_key, 6), position), (parts,), jnp.float32, smallest / len(cuts), largest / len(cuts))
        return jnp.repeat(jnp.exp(draws), extent[position] // parts).reshape((-1,) + (1,) * (len(extent) - position - 1))

    level = one(*cuts[0])
    for cut in cuts[1:]:
        level = level * one(*cut)
    return level


def noise(key, extent, deviation, most, cuts=(), kind=jnp.bfloat16):
    entries = jax.random.normal(key, extent, jnp.float32) * deviation
    if len(cuts) > 0:
        entries = steps_of(key, extent, cuts, -0.22, 0.18) * entries
    return jnp.clip(entries, min=-most, max=most).astype(kind)


def setup_inputs(seed: int = 0) -> dict:
    arg_keys = jax.random.split(jax.random.key(seed), 7)
    pair_rep = noise(arg_keys[0], (N, N, C), 1.0, 6.0, ((0, 4), (1, 8)))
    proj_weight = noise(arg_keys[1], (2, 4, C, H), C ** -0.5, 0.5)
    gate_weight = noise(arg_keys[2], (2, C, C), C ** -0.5, 0.5)
    out_weight = noise(arg_keys[3], (2, H, C), H ** -0.5, 0.5)
    in_gain = jnp.clip(1.0 + 0.18 * jax.random.normal(arg_keys[4], (2, C), jnp.float32), 0.1, 1.9)
    out_gain = jnp.clip(1.0 + 0.18 * jax.random.normal(arg_keys[5], (2, H), jnp.float32), 0.1, 1.9)
    return dict(pair_rep=pair_rep, proj_weight=proj_weight, gate_weight=gate_weight, out_weight=out_weight, in_gain=in_gain, out_gain=out_gain)


epsilon = 1e-05

def layer_norm(values, gain_row):
    center = values - lax.optimization_barrier(jnp.mean(values, axis=-1, keepdims=True))
    spread = lax.optimization_barrier(jnp.mean(center * center, axis=-1, keepdims=True))
    return center * lax.rsqrt(spread + epsilon) * gain_row

def reference(pair_rep, proj_weight, gate_weight, out_weight, in_gain, out_gain):
    row_block = math.gcd(N, 64)
    channel_block = math.gcd(H, 16)
    current = pair_rep
    for update_index in range(2):
        weight_joined = jnp.transpose(proj_weight[update_index], (1, 0, 2)).reshape(C, 4 * H)

        def project(row_slab):
            widened = row_slab.astype(jnp.float32)
            normed = layer_norm(widened, in_gain[update_index]).astype(jnp.bfloat16)
            projected = jnp.dot(normed, weight_joined, preferred_element_type=jnp.float32)
            left_hand = (jax.nn.sigmoid(projected[..., 0:H]) * projected[..., H:2 * H]).astype(jnp.bfloat16)
            right_hand = (jax.nn.sigmoid(projected[..., 2 * H:3 * H]) * projected[..., 3 * H:4 * H]).astype(jnp.bfloat16)
            gating = jax.nn.sigmoid(jnp.dot(normed, gate_weight[update_index], preferred_element_type=jnp.float32))
            return (left_hand, right_hand, gating)
        blocks = current.reshape(N // row_block, row_block, N, C)
        left_hand, right_hand, gating = lax.map(project, blocks)
        left_channels = jnp.moveaxis(left_hand.reshape(N, N, H), 2, 0).reshape(H // channel_block, channel_block, N, N)
        right_channels = jnp.moveaxis(right_hand.reshape(N, N, H), 2, 0).reshape(H // channel_block, channel_block, N, N)
        pattern = 'hik,hjk->hij' if update_index == 0 else 'hki,hkj->hij'

        def contract(operands):
            return jnp.einsum(pattern, operands[0].astype(jnp.float32), operands[1].astype(jnp.float32)).astype(jnp.bfloat16)
        triangle = lax.map(contract, (left_channels, right_channels))
        triangle = jnp.moveaxis(triangle.reshape(H, N, N), 0, 2)

        def finish(pieces):
            triangle_rows, gate_rows, old_rows = pieces
            mixed = layer_norm(triangle_rows.astype(jnp.float32), out_gain[update_index]).astype(jnp.bfloat16)
            update = jnp.dot(mixed, out_weight[update_index], preferred_element_type=jnp.float32)
            return (old_rows.astype(jnp.float32) + gate_rows * update).astype(jnp.bfloat16)
        current = lax.map(finish, (triangle.reshape(N // row_block, row_block, N, H), gating, blocks)).reshape(N, N, C)
    return current
```

```python
import functools

import jax
import jax.numpy as jnp
from jax import lax
from jax.experimental import pallas as pl
from jax.experimental.pallas import tpu as pltpu
from jax.sharding import PartitionSpec as P

epsilon = 1e-05
LANES = 128
PACK = 16
CHUNK = 16
f32 = jnp.float32
bf16 = jnp.bfloat16


def layer_norm(values, gain_row, reduce_axis):
    center = values - jnp.mean(values, axis=reduce_axis, keepdims=True)
    spread = jnp.mean(center * center, axis=reduce_axis, keepdims=True)
    return center * lax.rsqrt(spread + epsilon) * gain_row


def plain(pair_rep, proj_weight, gate_weight, out_weight, in_gain, out_gain):
    current = pair_rep
    for update_index in range(2):
        widened = current.astype(f32)
        normed = layer_norm(widened, in_gain[update_index], 2).astype(bf16)
        projected = jnp.einsum(
            "ijc,pch->phij", normed, proj_weight[update_index], preferred_element_type=f32
        )
        left_hand = (jax.nn.sigmoid(projected[0]) * projected[1]).astype(bf16)
        right_hand = (jax.nn.sigmoid(projected[2]) * projected[3]).astype(bf16)
        gating = jax.nn.sigmoid(
            jnp.dot(normed, gate_weight[update_index], preferred_element_type=f32)
        )
        left_rows, right_rows = (
            lax.all_to_all(left_hand, "col", split_axis=0, concat_axis=2, tiled=True),
            lax.all_to_all(right_hand, "col", split_axis=0, concat_axis=2, tiled=True),
        )
        if update_index == 0:
            triangle = jnp.einsum(
                "gik,gjk->igj",
                left_rows,
                lax.all_gather(right_rows, "row", axis=1, tiled=True),
                preferred_element_type=f32,
            )
        else:
            left_columns = lax.all_to_all(left_rows, "row", split_axis=2, concat_axis=1, tiled=True)
            triangle = jnp.einsum(
                "gki,gkj->igj",
                left_columns,
                lax.all_gather(right_rows, "row", axis=1, tiled=True),
                preferred_element_type=f32,
            )
        returned = lax.all_to_all(
            triangle.astype(bf16), "col", split_axis=2, concat_axis=1, tiled=True
        )
        mixed_rows = layer_norm(
            returned.astype(f32), out_gain[update_index][None, :, None], 1
        ).astype(bf16)
        update = jnp.einsum(
            "ihj,hc->ijc", mixed_rows, out_weight[update_index], preferred_element_type=f32
        )
        current = (widened + gating * update).astype(bf16)
    return current


def norm_columns(values, gain_column):
    scale = 1.0 / values.shape[0]
    center = values - jnp.sum(values, axis=0, keepdims=True) * scale
    spread = jnp.sum(center * center, axis=0, keepdims=True) * scale
    return center * lax.rsqrt(spread + epsilon) * gain_column


def layer_of(chunk):
    return 0 if chunk % 4 == 1 else 1


def kernel(rows, cols, x_ref, pw_ref, gw_ref, ow_ref, ig_ref, og_ref, o_ref,
           xt, nt, gt, tt, wt, gwt, owt, perm, shuffle, back,
           sa, sb, s1, ra, rb, r1, ml, mr, po, sp, rp, st0, rt0,
           rl, lo, rr, lx, tri, st1, rt1, sems):
    first, second, channels = x_ref.shape
    hidden = ow_ref.shape[1]
    side = cols // 2
    team = rows * side
    fold = LANES // second
    part = first // 2
    depth = part // fold
    block = CHUNK
    chunks = hidden // block
    owners = 2 * rows
    each = block // owners
    high = each * depth
    span = depth * LANES
    width = 2 * span
    step = min(span, 512)
    my_row, my_col = lax.axis_index("row"), lax.axis_index("col")
    my_half, my_side = my_col // side, my_col % side
    my_core, my_layer = my_col % 2, my_side // 2
    my_depth = my_layer + my_half - 2 * my_layer * my_half
    facing = (cols // 2 - 1 - my_col // 2) * 2 + my_core
    me = my_row * side + my_side
    mine = my_row * 2 + my_core
    HA, HB, H1, MT, ML, T0, T1 = 0, 1, 2, 4, 6, 8, 10

    barrier = pltpu.get_barrier_semaphore()

    def greet(row, col):
        pl.semaphore_signal(
            barrier, inc=1, device_id=(row, col), device_id_type=pl.DeviceIdType.MESH
        )

    def mate(n):
        return (my_row + n % rows) % rows, (my_side + n // rows) % side

    greet(my_row, facing)

    @pl.loop(1, team)
    def _(n):
        row, place = mate(n)
        greet(row, my_half * side + place)

    def send(source, target, kind, slot, row, col):
        pltpu.make_async_remote_copy(
            src_ref=source,
            dst_ref=target,
            send_sem=sems.at[2 * kind, slot],
            recv_sem=sems.at[2 * kind + 1, slot],
            device_id=(row, col),
            device_id_type=pl.DeviceIdType.MESH,
        ).start()

    def keep(source, target, kind, slot):
        pltpu.make_async_copy(source, target, sems.at[2 * kind + 1, slot]).start()

    def arrive(buffer, kind, slot):
        pltpu.make_async_copy(buffer, buffer, sems.at[2 * kind + 1, slot]).wait()

    def gone(buffer, kind, slot):
        pltpu.make_async_copy(buffer, buffer, sems.at[2 * kind, slot]).wait()

    def owned(c):
        return my_depth == layer_of(c)

    def spread(source, target, kind, c):
        o = layer_of(c)
        left = my_half * side + 2 * (o + my_half - 2 * o * my_half)

        def go(n):
            row, core = (my_row + n % rows) % rows, (my_core + n // rows) % 2
            send(source.at[c, row * 2 + core], target.at[c, me], kind, c, row, left + core)

        @pl.when(owned(c))
        def _():
            keep(source.at[c, mine], target.at[c, me], kind, c)

        @pl.when(jnp.logical_not(owned(c)))
        def _():
            go(0)

        @pl.loop(1, owners)
        def _(n):
            go(n)

    def give_back(source, target, kind, c):
        keep(source.at[c, me], target.at[c, mine], kind, c)

        @pl.loop(1, team)
        def _(n):
            row, place = mate(n)
            send(
                source.at[c, row * side + place], target.at[c, mine], kind, c,
                row, my_half * side + place,
            )

    def weight_turn(u):
        for p in range(4):
            turned = pw_ref[u, p].astype(f32).T.astype(bf16)
            for c in range(chunks):
                wt[u, c, p * block:(p + 1) * block, :] = turned[c * block:(c + 1) * block]

    def rest_of_setup():
        weight_turn(1)
        for u in range(2):
            gwt[u] = gw_ref[u].astype(f32).T.astype(bf16)
            owt[u] = ow_ref[u].astype(f32).T.astype(bf16)
        size = fold * LANES
        bits, low = LANES.bit_length() - 1, second.bit_length() - 1
        to = lax.broadcasted_iota(jnp.int32, (1, size), 1)
        at = lax.broadcasted_iota(jnp.int32, (size, size), 0)
        wanted = (
            (((to & (LANES - 1)) >> low) << bits) + ((to >> bits) << low) + (to & (second - 1))
        )
        perm[...] = jnp.where(at == wanted, 1.0, 0.0).astype(bf16)

    def regroup(parts):
        wide = jnp.concatenate([jnp.concatenate(tiles, axis=1) for tiles in parts], axis=0)
        return jnp.dot(wide, perm[...], preferred_element_type=f32)

    def unfold(get, matrices):
        moved = regroup([
            [get(r * side + p, s) for p in range(side)]
            for s in range(len(matrices)) for r in range(rows)
        ])
        for s, put in enumerate(matrices):
            for r in range(rows):
                at = (s * rows + r) * high
                for e in range(each):
                    put(e, r, jnp.concatenate([
                        moved[at + e * depth:at + (e + 1) * depth, a * LANES:(a + 1) * LANES]
                        for a in range(fold)
                    ], axis=0).astype(bf16))

    def refold(pick, put):
        moved = regroup([
            [
                jnp.concatenate([pick(e, r, a) for e in range(each)], axis=0).astype(bf16)
                for a in range(fold)
            ]
            for r in range(rows)
        ])
        for r in range(rows):
            for p in range(side):
                put(r * side + p, moved[
                    r * high:(r + 1) * high, p * LANES:(p + 1) * LANES
                ].astype(bf16))

    def columns(hf):
        return range(hf * span, (hf + 1) * span, step)

    def gain_of(ref, u):
        return jnp.broadcast_to(ref[u:u + 1, :], (LANES, LANES)).T[:, :1]

    def enter(u, hf):
        gain = gain_of(ig_ref, u)
        for t in columns(hf):
            nt[:, t:t + step] = norm_columns(xt[:, t:t + step], gain).astype(bf16)

    def project(u, c, hf):
        for t in columns(hf):
            got = jnp.dot(wt[u, c], nt[:, t:t + step], preferred_element_type=f32)
            for s in range(2):
                base = 2 * s * block
                hand = jax.nn.sigmoid(got[base:base + block]) * got[base + block:base + 2 * block]
                for k in range(step // LANES):
                    q = (t - hf * span) // LANES + k
                    shuffle[hf, s, pl.ds(q, block, stride=depth), :] = (
                        hand[:, k * LANES:(k + 1) * LANES]
                    )
        return [shuffle[hf, s].reshape(owners, high, LANES).astype(bf16) for s in range(2)]

    def open_gate(u, hf):
        for t in columns(hf):
            gt[:, t:t + step] = jax.nn.sigmoid(
                jnp.dot(gwt[u], nt[:, t:t + step], preferred_element_type=f32)
            )

    def lay(c, hf, got):
        back[...] = got.astype(f32).reshape(block * depth, LANES)
        for q in range(depth):
            t = hf * span + q * LANES
            tt[c * block:(c + 1) * block, t:t + LANES] = back[pl.ds(q, block, stride=depth), :]

    def leave(u, hf):
        gain = gain_of(og_ref, u)
        for t in columns(hf):
            mixed = norm_columns(tt[:, t:t + step], gain).astype(bf16)
            update = jnp.dot(owt[u], mixed, preferred_element_type=f32)
            xt[:, t:t + step] = (
                (xt[:, t:t + step] + gt[:, t:t + step] * update).astype(bf16).astype(f32)
            )

    own_rows = pl.ds(pl.multiple_of(my_half * LANES, LANES), LANES)
    far_rows = pl.ds(pl.multiple_of((1 - my_half) * LANES, LANES), LANES)

    def to_left(e, r, rows_of):
        ml[e, r * part:(r + 1) * part, :] = rows_of

    def to_right(c, hf):
        def put(e, r, rows_of):
            mr[c, e, r * first + hf * part:r * first + (hf + 1) * part, :] = rows_of
        return put

    def to_block(buffer, c, hf):
        def put(e, r, rows_of):
            at = (hf * rows + r) * part
            buffer[c, e, at:at + part, :] = rows_of
        return put

    def multiply(c, hf):
        over = (((1,), (1,)), ((), ()))

        @pl.when(owned(c))
        def _():
            if hf == 0:
                arrive(ra.at[c], HA, c)
                unfold(lambda d, s: ra[c, d, s], [to_left, to_right(c, 0), to_right(c, 1)])
            else:
                arrive(rb.at[c], HB, c)
                unfold(lambda d, s: rb[c, d], [to_left])
            for e in range(each):
                sp[hf, c, e] = lax.dot_general(
                    ml[e], mr[c, e, far_rows], over, preferred_element_type=f32
                ).astype(bf16)
            send(sp.at[hf, c], rp.at[hf, c], MT + hf, c, my_row, facing)
            for e in range(each):
                po[hf, c, e] = lax.dot_general(
                    ml[e], mr[c, e, own_rows], over, preferred_element_type=f32
                )

    def total(c, hf):
        @pl.when(owned(c))
        def _():
            arrive(rp.at[hf, c], MT + hf, c)

            def pick(e, r, a):
                at = (r * fold + a) * depth
                return po[hf, c, e, at:at + depth] + rp_wide[e][at:at + depth]

            rp_wide = [rp[hf, c, e].astype(f32) for e in range(each)]

            def put(d, tile):
                st0[hf, c, d] = tile

            refold(pick, put)
            give_back(st0.at[hf], rt0.at[hf], T0 + hf, c)

    def pass_on(c, hf):
        @pl.when(owned(c))
        def _():
            arrive(r1.at[hf, c], H1 + hf, c)
            send(r1.at[hf, c, :, 0], rl.at[hf, c], ML + hf, c, my_row, facing)

    def take_near(c, hf):
        @pl.when(owned(c))
        def _():
            unfold(lambda d, s: r1[hf, c, d, s], [to_block(lo, c, hf), to_block(rr, c, hf)])

    def take_far(c, hf):
        @pl.when(owned(c))
        def _():
            arrive(rl.at[hf, c], ML + hf, c)
            unfold(lambda d, s: rl[hf, c, d], [to_block(lx, c, hf)])

    def contract(c):
        over = (((0,), (0,)), ((), ()))

        @pl.when(owned(c))
        def _():
            for e in range(each):
                tri[e, own_rows, :] = lax.dot_general(
                    lo[c, e], rr[c, e], over, preferred_element_type=f32
                )
                tri[e, far_rows, :] = lax.dot_general(
                    lx[c, e], rr[c, e], over, preferred_element_type=f32
                )
            for hf in range(2):
                def pick(e, r, a):
                    at = r * first + hf * part + a * depth
                    return tri[e, at:at + depth, :]

                def put(d, tile):
                    st1[c, d, hf] = tile

                refold(pick, put)
            give_back(st1, rt1, T1, c)

    def collect(hf):
        for c in range(chunks):
            arrive(rt0.at[hf, c], T0 + hf, c)
            lay(c, hf, rt0[hf, c])
        leave(0, hf)
        enter(1, hf)

    def hand_over(c, hf):
        left, right = project(1, c, hf)
        s1[hf, c, :, 0] = left
        s1[hf, c, :, 1] = right
        spread(s1.at[hf], r1.at[hf], H1 + hf, c)

    weight_turn(0)
    for hf in range(2):
        for q in range(depth):
            tile = jnp.concatenate(
                [x_ref[hf * part + a * depth + q] for a in range(fold)], axis=0
            )
            t = hf * span + q * LANES
            xt[:, t:t + LANES] = tile.astype(f32).T
        enter(0, hf)
    for c in range(chunks):
        for hf in range(2):
            left, right = project(0, c, hf)
            if hf == 0:
                sa[c, :, 0] = left
            else:
                sb[c] = left
            sa[c, :, 1 + hf] = right
        if c == 0:
            pl.semaphore_wait(barrier, team)
        spread(sa, ra, HA, c)
    for c in range(chunks):
        spread(sb, rb, HB, c)
    rest_of_setup()
    for hf in range(2):
        open_gate(0, hf)
    lag = min(2, chunks)
    for c in range(chunks):
        multiply(c, 0)
        if c >= lag:
            total(c - lag, 0)
    for c in range(chunks):
        multiply(c, 1)
        if c < lag:
            total(chunks - lag + c, 0)
    collect(0)
    for c in range(chunks):
        hand_over(c, 0)
        total(c, 1)
        if c >= lag:
            pass_on(c - lag, 0)
    for c in range(chunks - lag, chunks):
        pass_on(c, 0)
    open_gate(1, 0)
    collect(1)
    for c in range(chunks):
        hand_over(c, 1)
        take_near(c, 0)
        if c >= lag:
            pass_on(c - lag, 1)
    for c in range(chunks - lag, chunks):
        pass_on(c, 1)
    open_gate(1, 1)
    for c in range(chunks):
        take_far(c, 0)
        take_near(c, 1)
    for c in range(chunks):
        take_far(c, 1)
        contract(c)
    for c in range(chunks):
        arrive(rt1.at[c], T1, c)
        for hf in range(2):
            lay(c, hf, rt1[c, :, hf])
    for hf in range(2):
        leave(1, hf)
    o_ref[...] = xt[...].astype(bf16)

    for c in range(chunks):
        @pl.when(owned(c))
        def _():
            most = pl.ds(0, owners - 1)
            gone(sa.at[c, most], HA, c)
            gone(sb.at[c, most], HB, c)
            for hf in range(2):
                gone(s1.at[hf, c, most], H1 + hf, c)
                gone(sp.at[hf, c], MT + hf, c)
                gone(rl.at[hf, c], ML + hf, c)
                gone(st0.at[hf, c, pl.ds(0, team - 1)], T0 + hf, c)
            gone(st1.at[c, pl.ds(0, team - 1)], T1, c)

        @pl.when(jnp.logical_not(owned(c)))
        def _():
            gone(sa.at[c], HA, c)
            gone(sb.at[c], HB, c)
            for hf in range(2):
                gone(s1.at[hf, c], H1 + hf, c)


def finish(fold, t_ref, o_ref):
    first, second, _ = o_ref.shape
    part = first // 2
    depth = part // fold
    for hf in range(2):
        for q in range(depth):
            t = (hf * depth + q) * LANES
            tile = t_ref[:, t:t + LANES].astype(f32).T.astype(bf16)
            for a in range(fold):
                o_ref[hf * part + a * depth + q] = tile[a * second:(a + 1) * second]


def takes(rows, cols, first, second, channels, hidden):
    if LANES % second or channels != LANES or hidden != LANES or cols % 4 or first % 2:
        return False
    fold, owners = LANES // second, 2 * rows
    return (
        cols // 2 == fold and cols // 4 == 2 and CHUNK % owners == 0
        and (first // 2) % fold == 0 and rows * first == cols * second
        and first // 2 // fold == 8 and CHUNK // owners * 8 == PACK
    )


def solution(mesh):
    rows, cols = mesh.shape["row"], mesh.shape["col"]

    def local(pair_rep, proj_weight, gate_weight, out_weight, in_gain, out_gain):
        first, second, channels = pair_rep.shape
        hidden = out_weight.shape[1]
        args = (pair_rep, proj_weight, gate_weight, out_weight, in_gain, out_gain)
        if not takes(rows, cols, first, second, channels, hidden):
            return plain(*args)
        team, owners = rows * (cols // 2), 2 * rows
        fold = LANES // second
        depth = first // 2 // fold
        chunks = hidden // CHUNK
        each = CHUNK // owners
        high = each * depth
        width = 2 * depth * LANES
        vmem = pl.BlockSpec(memory_space=pltpu.VMEM)
        turned = pl.pallas_call(
            functools.partial(kernel, rows, cols),
            out_shape=jax.ShapeDtypeStruct((channels, width), bf16),
            in_specs=[vmem] * 6,
            out_specs=vmem,
            scratch_shapes=[
                pltpu.VMEM((channels, width), f32),
                pltpu.VMEM((channels, width), bf16),
                pltpu.VMEM((channels, width), f32),
                pltpu.VMEM((hidden, width), f32),
                pltpu.VMEM((2, chunks, 4 * CHUNK, channels), bf16),
                pltpu.VMEM((2, channels, channels), bf16),
                pltpu.VMEM((2, channels, hidden), bf16),
                pltpu.VMEM((fold * LANES, fold * LANES), bf16),
                pltpu.VMEM((2, 2, CHUNK * depth, LANES), f32),
                pltpu.VMEM((CHUNK * depth, LANES), f32),
                pltpu.VMEM((chunks, owners, 3, high, LANES), bf16),
                pltpu.VMEM((chunks, owners, high, LANES), bf16),
                pltpu.VMEM((2, chunks, owners, 2, high, LANES), bf16),
                pltpu.VMEM((chunks, team, 3, high, LANES), bf16),
                pltpu.VMEM((chunks, team, high, LANES), bf16),
                pltpu.VMEM((2, chunks, team, 2, high, LANES), bf16),
                pltpu.VMEM((each, LANES, LANES), bf16),
                pltpu.VMEM((chunks, each, 2 * LANES, LANES), bf16),
                pltpu.VMEM((2, chunks, each, LANES, LANES), f32),
                pltpu.VMEM((2, chunks, each, LANES, LANES), bf16),
                pltpu.VMEM((2, chunks, each, LANES, LANES), bf16),
                pltpu.VMEM((2, chunks, team, high, LANES), bf16),
                pltpu.VMEM((2, chunks, owners, high, LANES), bf16),
                pltpu.VMEM((2, chunks, team, high, LANES), bf16),
                pltpu.VMEM((chunks, each, 2 * LANES, LANES), bf16),
                pltpu.VMEM((chunks, each, 2 * LANES, LANES), bf16),
                pltpu.VMEM((chunks, each, 2 * LANES, LANES), bf16),
                pltpu.VMEM((each, 2 * LANES, LANES), f32),
                pltpu.VMEM((chunks, team, 2, high, LANES), bf16),
                pltpu.VMEM((chunks, owners, 2, high, LANES), bf16),
                pltpu.SemaphoreType.DMA((22, chunks)),
            ],
            compiler_params=pltpu.CompilerParams(collective_id=0, has_side_effects=True),
        )(*args)
        return pl.pallas_call(
            functools.partial(finish, fold),
            out_shape=jax.ShapeDtypeStruct(pair_rep.shape, bf16),
            in_specs=[vmem],
            out_specs=vmem,
        )(turned)

    return jax.shard_map(
        local,
        mesh=mesh,
        in_specs=(P("row", "col", None), P(), P(), P(), P(), P()),
        out_specs=P("row", "col", None),
        check_vma=False,
    )
```

```python
import functools

import jax
import jax.numpy as jnp
from jax import lax
from jax.experimental import pallas as pl
from jax.experimental.pallas import tpu as pltpu
from jax.sharding import PartitionSpec as P

epsilon = 1e-05
LANES = 128
PACK = 16
CHUNK = 16
f32 = jnp.float32
bf16 = jnp.bfloat16


def layer_norm(values, gain_row, reduce_axis):
    center = values - jnp.mean(values, axis=reduce_axis, keepdims=True)
    spread = jnp.mean(center * center, axis=reduce_axis, keepdims=True)
    return center * lax.rsqrt(spread + epsilon) * gain_row


def plain(pair_rep, proj_weight, gate_weight, out_weight, in_gain, out_gain):
    current = pair_rep
    for update_index in range(2):
        widened = current.astype(f32)
        normed = layer_norm(widened, in_gain[update_index], 2).astype(bf16)
        projected = jnp.einsum(
            "ijc,pch->phij", normed, proj_weight[update_index], preferred_element_type=f32
        )
        left_hand = (jax.nn.sigmoid(projected[0]) * projected[1]).astype(bf16)
        right_hand = (jax.nn.sigmoid(projected[2]) * projected[3]).astype(bf16)
        gating = jax.nn.sigmoid(
            jnp.dot(normed, gate_weight[update_index], preferred_element_type=f32)
        )
        left_rows, right_rows = (
            lax.all_to_all(left_hand, "col", split_axis=0, concat_axis=2, tiled=True),
            lax.all_to_all(right_hand, "col", split_axis=0, concat_axis=2, tiled=True),
        )
        if update_index == 0:
            triangle = jnp.einsum(
                "gik,gjk->igj",
                left_rows,
                lax.all_gather(right_rows, "row", axis=1, tiled=True),
                preferred_element_type=f32,
            )
        else:
            left_columns = lax.all_to_all(left_rows, "row", split_axis=2, concat_axis=1, tiled=True)
            triangle = jnp.einsum(
                "gki,gkj->igj",
                left_columns,
                lax.all_gather(right_rows, "row", axis=1, tiled=True),
                preferred_element_type=f32,
            )
        returned = lax.all_to_all(
            triangle.astype(bf16), "col", split_axis=2, concat_axis=1, tiled=True
        )
        mixed_rows = layer_norm(
            returned.astype(f32), out_gain[update_index][None, :, None], 1
        ).astype(bf16)
        update = jnp.einsum(
            "ihj,hc->ijc", mixed_rows, out_weight[update_index], preferred_element_type=f32
        )
        current = (widened + gating * update).astype(bf16)
    return current


def norm_columns(values, gain_column):
    scale = 1.0 / values.shape[0]
    center = values - jnp.sum(values, axis=0, keepdims=True) * scale
    spread = jnp.sum(center * center, axis=0, keepdims=True) * scale
    return center * lax.rsqrt(spread + epsilon) * gain_column


def kernel(rows, cols, x_ref, pw_ref, gw_ref, ow_ref, ig_ref, og_ref, o_ref,
           xt, nt, gt, tt, wt, gwt, owt, perm, shuffle, back,
           send_h, recv_h0, recv_l1, recv_r1, send_t0, recv_t0, send_t1, recv_t1, ml, mr, sems, ready):
    first, second, channels = x_ref.shape
    hidden = ow_ref.shape[1]
    side = cols // 2
    team = rows * side
    fold = LANES // second
    depth = first // fold
    block = CHUNK
    chunks = hidden // block
    each = block // team
    groups = side // fold
    width = depth * LANES
    step = min(width, 512)
    my_row, my_col = lax.axis_index("row"), lax.axis_index("col")
    my_half, my_side = my_col // side, my_col % side
    me = my_row * side + my_side

    def mate(n):
        m = (n * 13) % team if team % 13 else n
        row, place = (my_row + m % rows) % rows, (my_side + m // rows) % side
        return row, place

    def device(n, other):
        row, place = mate(n)
        return row, (1 - my_half if other else my_half) * side + place

    barrier = pltpu.get_barrier_semaphore()

    def greet(n, other):
        pl.semaphore_signal(
            barrier, inc=1, device_id=device(n, other), device_id_type=pl.DeviceIdType.MESH
        )

    greet(0, True)

    @pl.loop(1, team)
    def _(n):
        greet(n, False)

    def send(source, target, kind, slot, n, other):
        row, place = mate(n)
        pltpu.make_async_remote_copy(
            src_ref=source(row, place, other),
            dst_ref=target,
            send_sem=sems.at[2 * kind, slot],
            recv_sem=sems.at[2 * kind + 1, slot],
            device_id=device(n, other),
            device_id_type=pl.DeviceIdType.MESH,
        ).start()

    def keep(source, target, kind, slot):
        pltpu.make_async_copy(
            source(my_row, my_side, False), target, sems.at[2 * kind + 1, slot]
        ).start()

    def arrive(buffer, kind, slot):
        pltpu.make_async_copy(buffer, buffer, sems.at[2 * kind + 1, slot]).wait()

    def weight_turn(u):
        for p in range(4):
            turned = pw_ref[u, p].astype(f32).T.astype(bf16)
            for c in range(chunks):
                wt[u, c, p * block:(p + 1) * block, :] = turned[c * block:(c + 1) * block]

    weight_turn(0)
    for q in range(depth):
        tile = jnp.concatenate([x_ref[a * depth + q] for a in range(fold)], axis=0)
        xt[:, q * LANES:(q + 1) * LANES] = tile.astype(f32).T

    def rest_of_setup():
        weight_turn(1)
        for u in range(2):
            gwt[u] = gw_ref[u].astype(f32).T.astype(bf16)
            owt[u] = ow_ref[u].astype(f32).T.astype(bf16)
        size = fold * LANES
        bits, low = LANES.bit_length() - 1, second.bit_length() - 1
        to = lax.broadcasted_iota(jnp.int32, (1, size), 1)
        at = lax.broadcasted_iota(jnp.int32, (size, size), 0)
        wanted = (
            (((to & (LANES - 1)) >> low) << bits) + ((to >> bits) << low) + (to & (second - 1))
        )
        perm[...] = jnp.where(at == wanted, 1.0, 0.0).astype(bf16)

    def regroup(parts):
        wide = jnp.concatenate([jnp.concatenate(tiles, axis=0) for tiles in parts], axis=1)
        return jnp.dot(wide, perm[...], preferred_element_type=f32).astype(bf16)

    def tile_of(array, row, lane):
        return array[row * depth:(row + 1) * depth, lane * LANES:(lane + 1) * LANES]

    for u in range(2):
        gain_in = jnp.broadcast_to(ig_ref[u:u + 1, :], (LANES, channels)).T[:, :1]
        gain_out = jnp.broadcast_to(og_ref[u:u + 1, :], (LANES, hidden)).T[:, :1]
        for t in range(0, width, step):
            nt[:, t:t + step] = norm_columns(xt[:, t:t + step], gain_in).astype(bf16)
        for c in range(chunks):
            for t in range(0, width, step):
                got = jnp.dot(wt[u, c], nt[:, t:t + step], preferred_element_type=f32)
                for s in range(2):
                    base = 2 * s * block
                    hand = jax.nn.sigmoid(got[base:base + block]) * got[base + block:base + 2 * block]
                    for k in range(step // LANES):
                        shuffle[s, pl.ds(t // LANES + k, block, stride=depth), :] = (
                            hand[:, k * LANES:(k + 1) * LANES]
                        )
            for s in range(2):
                send_h[u, c, :, s] = shuffle[s].reshape(team, each, depth, LANES).astype(bf16)
            if u == 0:
                if c == 0:
                    pl.semaphore_wait(barrier, team)
                    pl.semaphore_signal(
                        ready, inc=1, device_id=device(0, True),
                        device_id_type=pl.DeviceIdType.MESH,
                    )
                both = lambda row, place, other: send_h.at[0, c, row * side + place]
                keep(both, recv_h0.at[c, me], 0, c)

                @pl.loop(1, team)
                def _(n):
                    send(both, recv_h0.at[c, me], 0, c, n, False)
            else:
                left = lambda row, place, other: send_h.at[1, c, row * side + place, 0]
                right = lambda row, place, other: send_h.at[1, c, row * side + place, 1]
                keep(left, recv_l1.at[c, my_half * team + me], 1, c)
                keep(right, recv_r1.at[c, me], 2, c)
                send(left, recv_l1.at[c, my_half * team + me], 1, c, 0, True)

                @pl.loop(1, team)
                def _(n):
                    send(left, recv_l1.at[c, my_half * team + me], 1, c, n, True)
                    send(left, recv_l1.at[c, my_half * team + me], 1, c, n, False)
                    send(right, recv_r1.at[c, me], 2, c, n, False)
        if u == 0:
            rest_of_setup()
        for t in range(0, width, step):
            gt[:, t:t + step] = jax.nn.sigmoid(
                jnp.dot(gwt[u], nt[:, t:t + step], preferred_element_type=f32)
            )
        for c in range(chunks):
            if u == 0:
                arrive(recv_h0.at[c], 0, c)
                sources = [
                    (matrix, e, 0, lambda d, s=s, e=e: recv_h0[c, d, s, e])
                    for s, matrix in enumerate((ml, mr)) for e in range(each)
                ]
            else:
                arrive(recv_l1.at[c], 1, c)
                arrive(recv_r1.at[c], 2, c)
                sources = [
                    (ml, e, h, lambda d, h=h, e=e: recv_l1[c, h * team + d, e])
                    for h in range(2) for e in range(each)
                ] + [(mr, e, 0, lambda d, e=e: recv_r1[c, d, e]) for e in range(each)]
            moved = regroup([
                [
                    get(r * side + g * fold + i)
                    for _, _, _, get in sources for r in range(rows) for g in range(groups)
                ]
                for i in range(fold)
            ])
            at = 0
            for matrix, e, h, _ in sources:
                for r in range(rows):
                    for g in range(groups):
                        lane = (h * groups + g) * LANES
                        for a in range(fold):
                            matrix[e, r * first + a * depth:r * first + (a + 1) * depth,
                                   lane:lane + LANES] = tile_of(moved, at, a)
                        at += 1
            wide_groups = 2 * groups if u == 0 else groups
            triangles = []
            for e in range(each):
                if u == 0:
                    pair = ml[e, :, :groups * LANES], mr[e]
                    over = (((1,), (1,)), ((), ()))
                else:
                    pair = ml[e], mr[e]
                    over = (((0,), (0,)), ((), ()))
                triangles.append(
                    lax.dot_general(*pair, over, preferred_element_type=f32).astype(bf16)
                )
            moved = regroup([
                [
                    tile_of(triangles[e], r * fold + a, g)
                    for e in range(each) for r in range(rows) for g in range(wide_groups)
                ]
                for a in range(fold)
            ])
            at = 0
            out = send_t0 if u == 0 else send_t1
            for e in range(each):
                for r in range(rows):
                    for g in range(wide_groups):
                        for i in range(fold):
                            place = g * fold + i
                            half, place = place // side, place % side
                            tile = tile_of(moved, at, i)
                            if u == 0:
                                out[c, half, r * side + place, e] = tile
                            else:
                                out[c, r * side + place, e] = tile
                        at += 1
            if u == 0:
                sums = lambda row, place, other: send_t0.at[
                    c, 1 - my_half if other else my_half, row * side + place
                ]
                keep(sums, recv_t0.at[c, my_half * team + me], 3, c)
                if c == 0:
                    pl.semaphore_wait(ready, 1)
                send(sums, recv_t0.at[c, my_half * team + me], 3, c, 0, True)

                @pl.loop(1, team)
                def _(n):
                    send(sums, recv_t0.at[c, my_half * team + me], 3, c, n, True)
                    send(sums, recv_t0.at[c, my_half * team + me], 3, c, n, False)
            else:
                made = lambda row, place, other: send_t1.at[c, row * side + place]
                keep(made, recv_t1.at[c, me], 4, c)

                @pl.loop(1, team)
                def _(n):
                    send(made, recv_t1.at[c, me], 4, c, n, False)
        for c in range(chunks):
            if u == 0:
                arrive(recv_t0.at[c], 3, c)
                total = recv_t0[c, :team].astype(f32) + recv_t0[c, team:].astype(f32)
            else:
                arrive(recv_t1.at[c], 4, c)
                total = recv_t1[c].astype(f32)
            back[...] = total.reshape(block * depth, LANES)
            for q in range(depth):
                tt[c * block:(c + 1) * block, q * LANES:(q + 1) * LANES] = (
                    back[pl.ds(q, block, stride=depth), :]
                )
        for t in range(0, width, step):
            mixed = norm_columns(tt[:, t:t + step], gain_out).astype(bf16)
            update = jnp.dot(owt[u], mixed, preferred_element_type=f32)
            xt[:, t:t + step] = (
                (xt[:, t:t + step] + gt[:, t:t + step] * update).astype(bf16).astype(f32)
            )
    o_ref[...] = xt[...].astype(bf16)

    def gone(buffer, kind, slot):
        pltpu.make_async_copy(buffer, buffer, sems.at[2 * kind, slot]).wait()

    for c in range(chunks):
        gone(recv_h0.at[c, pl.ds(0, team - 1)], 0, c)
        gone(recv_l1.at[c, pl.ds(0, 2 * team - 1)], 1, c)
        gone(recv_r1.at[c, pl.ds(0, team - 1)], 2, c)
        gone(recv_t0.at[c, pl.ds(0, 2 * team - 1)], 3, c)
        gone(recv_t1.at[c, pl.ds(0, team - 1)], 4, c)


def finish(fold, t_ref, o_ref):
    first, second, _ = o_ref.shape
    depth = first // fold
    for q in range(depth):
        tile = t_ref[:, q * LANES:(q + 1) * LANES].astype(f32).T.astype(bf16)
        for a in range(fold):
            o_ref[a * depth + q] = tile[a * second:(a + 1) * second]


def takes(rows, cols, first, second, channels, hidden):
    if LANES % second or channels != LANES or hidden != LANES or cols % 2:
        return False
    team, fold = rows * (cols // 2), LANES // second
    return (
        CHUNK % team == 0 and first % fold == 0 and (first // fold) % PACK == 0
        and (cols // 2) % fold == 0 and first * second <= 2048
    )


def solution(mesh):
    rows, cols = mesh.shape["row"], mesh.shape["col"]

    def local(pair_rep, proj_weight, gate_weight, out_weight, in_gain, out_gain):
        first, second, channels = pair_rep.shape
        hidden = out_weight.shape[1]
        args = (pair_rep, proj_weight, gate_weight, out_weight, in_gain, out_gain)
        if not takes(rows, cols, first, second, channels, hidden):
            return plain(*args)
        team = rows * (cols // 2)
        fold = LANES // second
        depth = first // fold
        chunks = hidden // CHUNK
        each = CHUNK // team
        width = depth * LANES
        vmem = pl.BlockSpec(memory_space=pltpu.VMEM)
        turned = pl.pallas_call(
            functools.partial(kernel, rows, cols),
            out_shape=jax.ShapeDtypeStruct((channels, width), bf16),
            in_specs=[vmem] * 6,
            out_specs=vmem,
            scratch_shapes=[
                pltpu.VMEM((channels, width), f32),
                pltpu.VMEM((channels, width), bf16),
                pltpu.VMEM((channels, width), f32),
                pltpu.VMEM((hidden, width), f32),
                pltpu.VMEM((2, chunks, 4 * CHUNK, channels), bf16),
                pltpu.VMEM((2, channels, channels), bf16),
                pltpu.VMEM((2, channels, hidden), bf16),
                pltpu.VMEM((fold * LANES, fold * LANES), bf16),
                pltpu.VMEM((2, CHUNK * depth, LANES), f32),
                pltpu.VMEM((CHUNK * depth, LANES), f32),
                pltpu.VMEM((2, chunks, team, 2, each, depth, LANES), bf16),
                pltpu.VMEM((chunks, team, 2, each, depth, LANES), bf16),
                pltpu.VMEM((chunks, 2 * team, each, depth, LANES), bf16),
                pltpu.VMEM((chunks, team, each, depth, LANES), bf16),
                pltpu.VMEM((chunks, 2, team, each, depth, LANES), bf16),
                pltpu.VMEM((chunks, 2 * team, each, depth, LANES), bf16),
                pltpu.VMEM((chunks, team, each, depth, LANES), bf16),
                pltpu.VMEM((chunks, team, each, depth, LANES), bf16),
                pltpu.VMEM((each, rows * first, cols * second), bf16),
                pltpu.VMEM((each, rows * first, cols // 2 * second), bf16),
                pltpu.SemaphoreType.DMA((10, chunks)),
                pltpu.SemaphoreType.REGULAR,
            ],
            compiler_params=pltpu.CompilerParams(collective_id=0, has_side_effects=True),
        )(*args)
        return pl.pallas_call(
            functools.partial(finish, fold),
            out_shape=jax.ShapeDtypeStruct(pair_rep.shape, bf16),
            in_specs=[vmem],
            out_specs=vmem,
        )(turned)

    return jax.shard_map(
        local,
        mesh=mesh,
        in_specs=(P("row", "col", None), P(), P(), P(), P(), P()),
        out_specs=P("row", "col", None),
        check_vma=False,
    )
```

```python
import functools

import jax
import jax.numpy as jnp
from jax import lax
from jax.experimental import pallas as pl
from jax.experimental.pallas import tpu as pltpu
from jax.sharding import PartitionSpec as P

epsilon = 1e-05
LANES = 128
PACK = 16
CHUNK = 32
f32 = jnp.float32
bf16 = jnp.bfloat16


def layer_norm(values, gain_row, reduce_axis):
    center = values - jnp.mean(values, axis=reduce_axis, keepdims=True)
    spread = jnp.mean(center * center, axis=reduce_axis, keepdims=True)
    return center * lax.rsqrt(spread + epsilon) * gain_row


def plain(pair_rep, proj_weight, gate_weight, out_weight, in_gain, out_gain):
    current = pair_rep
    for update_index in range(2):
        widened = current.astype(f32)
        normed = layer_norm(widened, in_gain[update_index], 2).astype(bf16)
        projected = jnp.einsum(
            "ijc,pch->phij", normed, proj_weight[update_index], preferred_element_type=f32
        )
        left_hand = (jax.nn.sigmoid(projected[0]) * projected[1]).astype(bf16)
        right_hand = (jax.nn.sigmoid(projected[2]) * projected[3]).astype(bf16)
        gating = jax.nn.sigmoid(
            jnp.dot(normed, gate_weight[update_index], preferred_element_type=f32)
        )
        left_rows, right_rows = (
            lax.all_to_all(left_hand, "col", split_axis=0, concat_axis=2, tiled=True),
            lax.all_to_all(right_hand, "col", split_axis=0, concat_axis=2, tiled=True),
        )
        if update_index == 0:
            triangle = jnp.einsum(
                "gik,gjk->igj",
                left_rows,
                lax.all_gather(right_rows, "row", axis=1, tiled=True),
                preferred_element_type=f32,
            )
        else:
            left_columns = lax.all_to_all(left_rows, "row", split_axis=2, concat_axis=1, tiled=True)
            triangle = jnp.einsum(
                "gki,gkj->igj",
                left_columns,
                lax.all_gather(right_rows, "row", axis=1, tiled=True),
                preferred_element_type=f32,
            )
        returned = lax.all_to_all(
            triangle.astype(bf16), "col", split_axis=2, concat_axis=1, tiled=True
        )
        mixed_rows = layer_norm(
            returned.astype(f32), out_gain[update_index][None, :, None], 1
        ).astype(bf16)
        update = jnp.einsum(
            "ihj,hc->ijc", mixed_rows, out_weight[update_index], preferred_element_type=f32
        )
        current = (widened + gating * update).astype(bf16)
    return current


def norm_columns(values, gain_column):
    scale = 1.0 / values.shape[0]
    center = values - jnp.sum(values, axis=0, keepdims=True) * scale
    spread = jnp.sum(center * center, axis=0, keepdims=True) * scale
    return center * lax.rsqrt(spread + epsilon) * gain_column


def kernel(rows, cols, x_ref, pw_ref, gw_ref, ow_ref, ig_ref, og_ref, o_ref,
           xt, nt, gt, tt, wt, gwt, owt, perm, shuffle, back,
           sa, sb, s1, ra, rb, rl, rr, ml, mr, st0, rt0, ll, lr, st1, rt1, sems, ready):
    first, second, channels = x_ref.shape
    hidden = ow_ref.shape[1]
    side = cols // 2
    team = rows * side
    fold = LANES // second
    part = first // 2
    depth = part // fold
    block = CHUNK
    chunks = hidden // block
    each = block // team
    high = each * depth
    span = depth * LANES
    width = 2 * span
    step = min(span, 512)
    my_row, my_col = lax.axis_index("row"), lax.axis_index("col")
    my_half, my_side = my_col // side, my_col % side
    me = my_row * side + my_side
    HA, HB, L1, R1, T0, T1 = 0, 1, 2, 4, 6, 8

    def mate(n):
        m = (n * 13) % team if team % 13 else n
        return (my_row + m % rows) % rows, (my_side + m // rows) % side

    def device(n, other):
        row, place = mate(n)
        return row, (1 - my_half if other else my_half) * side + place

    barrier = pltpu.get_barrier_semaphore()

    def greet(n, other):
        pl.semaphore_signal(
            barrier, inc=1, device_id=device(n, other), device_id_type=pl.DeviceIdType.MESH
        )

    greet(0, True)

    @pl.loop(1, team)
    def _(n):
        greet(n, False)

    def send(source, target, kind, slot, n, other):
        row, place = mate(n)
        pltpu.make_async_remote_copy(
            src_ref=source(row * side + place, other),
            dst_ref=target,
            send_sem=sems.at[2 * kind, slot],
            recv_sem=sems.at[2 * kind + 1, slot],
            device_id=device(n, other),
            device_id_type=pl.DeviceIdType.MESH,
        ).start()

    def arrive(buffer, kind, slot):
        pltpu.make_async_copy(buffer, buffer, sems.at[2 * kind + 1, slot]).wait()

    def gone(buffer, kind, slot):
        pltpu.make_async_copy(buffer, buffer, sems.at[2 * kind, slot]).wait()

    def spread(jobs, slot):
        for source, target, kind, across in jobs:
            pltpu.make_async_copy(
                source(me, False), target, sems.at[2 * kind + 1, slot]
            ).start()
            if across:
                send(source, target, kind, slot, 0, True)

        @pl.loop(1, team)
        def _(n):
            for source, target, kind, across in jobs:
                if across:
                    send(source, target, kind, slot, n, True)
                send(source, target, kind, slot, n, False)

    def weight_turn(u):
        for p in range(4):
            turned = pw_ref[u, p].astype(f32).T.astype(bf16)
            for c in range(chunks):
                wt[u, c, p * block:(p + 1) * block, :] = turned[c * block:(c + 1) * block]

    def rest_of_setup():
        weight_turn(1)
        for u in range(2):
            gwt[u] = gw_ref[u].astype(f32).T.astype(bf16)
            owt[u] = ow_ref[u].astype(f32).T.astype(bf16)
        size = fold * LANES
        bits, low = LANES.bit_length() - 1, second.bit_length() - 1
        to = lax.broadcasted_iota(jnp.int32, (1, size), 1)
        at = lax.broadcasted_iota(jnp.int32, (size, size), 0)
        wanted = (
            (((to & (LANES - 1)) >> low) << bits) + ((to >> bits) << low) + (to & (second - 1))
        )
        perm[...] = jnp.where(at == wanted, 1.0, 0.0).astype(bf16)

    def regroup(parts):
        wide = jnp.concatenate([jnp.concatenate(tiles, axis=1) for tiles in parts], axis=0)
        return jnp.dot(wide, perm[...], preferred_element_type=f32)

    def unfold(sources):
        moved = regroup([
            [get(r * side + p) for p in range(side)] for get, _ in sources for r in range(rows)
        ])
        for s, (_, put) in enumerate(sources):
            for r in range(rows):
                at = (s * rows + r) * high
                for e in range(each):
                    put(e, r, jnp.concatenate([
                        moved[at + e * depth:at + (e + 1) * depth, a * LANES:(a + 1) * LANES]
                        for a in range(fold)
                    ], axis=0).astype(bf16))

    def refold(targets):
        moved = regroup([
            [
                jnp.concatenate([pick(e, r, a) for e in range(each)], axis=0).astype(bf16)
                for a in range(fold)
            ]
            for pick, _ in targets for r in range(rows)
        ])
        for s, (_, put) in enumerate(targets):
            for r in range(rows):
                at = (s * rows + r) * high
                for p in range(side):
                    put(r * side + p, moved[
                        at:at + high, p * LANES:(p + 1) * LANES
                    ].astype(bf16))

    def columns(hf):
        return range(hf * span, (hf + 1) * span, step)

    def gain_of(ref, u):
        return jnp.broadcast_to(ref[u:u + 1, :], (LANES, LANES)).T[:, :1]

    def enter(u, hf):
        gain = gain_of(ig_ref, u)
        for t in columns(hf):
            nt[:, t:t + step] = norm_columns(xt[:, t:t + step], gain).astype(bf16)

    def project(u, c, hf):
        for t in columns(hf):
            got = jnp.dot(wt[u, c], nt[:, t:t + step], preferred_element_type=f32)
            for s in range(2):
                base = 2 * s * block
                hand = jax.nn.sigmoid(got[base:base + block]) * got[base + block:base + 2 * block]
                for k in range(step // LANES):
                    q = (t - hf * span) // LANES + k
                    shuffle[hf, s, pl.ds(q, block, stride=depth), :] = (
                        hand[:, k * LANES:(k + 1) * LANES]
                    )
        return [shuffle[hf, s].reshape(team, high, LANES).astype(bf16) for s in range(2)]

    def open_gate(u, hf):
        for t in columns(hf):
            gt[:, t:t + step] = jax.nn.sigmoid(
                jnp.dot(gwt[u], nt[:, t:t + step], preferred_element_type=f32)
            )

    def lay(c, hf, got):
        back[...] = got.reshape(block * depth, LANES)
        for q in range(depth):
            t = hf * span + q * LANES
            tt[c * block:(c + 1) * block, t:t + LANES] = back[pl.ds(q, block, stride=depth), :]

    def leave(u, hf):
        gain = gain_of(og_ref, u)
        for t in columns(hf):
            mixed = norm_columns(tt[:, t:t + step], gain).astype(bf16)
            update = jnp.dot(owt[u], mixed, preferred_element_type=f32)
            xt[:, t:t + step] = (
                (xt[:, t:t + step] + gt[:, t:t + step] * update).astype(bf16).astype(f32)
            )

    def into(buffer, hf):
        def put(e, r, rows_of):
            at = (hf * rows + r) * part
            buffer[e, at:at + part, :] = rows_of
        return put

    def to_left(e, r, rows_of):
        ml[e, r * part:(r + 1) * part, :] = rows_of

    def to_right(c, hf):
        def put(e, r, rows_of):
            at = r * first + hf * part
            mr[c, e, at:at + part, :] = rows_of
        return put

    def multiply(c, hf):
        if hf == 0:
            arrive(ra.at[c], HA, c)
            unfold([
                (lambda d: ra[c, d, 0], to_left),
                (lambda d: ra[c, d, 1], to_right(c, 0)),
                (lambda d: ra[c, d, 2], to_right(c, 1)),
            ])
        else:
            arrive(rb.at[c], HB, c)
            unfold([(lambda d: rb[c, d], to_left)])
        sums = [
            lax.dot_general(
                ml[e], mr[c, e], (((1,), (1,)), ((), ())), preferred_element_type=f32
            )
            for e in range(each)
        ]

        def piece(h):
            def pick(e, r, a):
                at = (r * fold + a) * depth
                return sums[e][at:at + depth, h * LANES:(h + 1) * LANES]

            def put(d, tile):
                st0[hf, c, h, d] = tile
            return pick, put

        refold([piece(h) for h in range(2)])
        if c == 0 and hf == 0:
            pl.semaphore_wait(ready, 1)
        spread([(
            lambda d, other: st0.at[hf, c, 1 - my_half if other else my_half, d],
            rt0.at[hf, c, my_half * team + me], T0 + hf, True,
        )], c)

    def collect(hf):
        for c in range(chunks):
            arrive(rt0.at[hf, c], T0 + hf, c)
            lay(c, hf, rt0[hf, c, :team].astype(f32) + rt0[hf, c, team:].astype(f32))
        leave(0, hf)
        enter(1, hf)

    def hand_over(c, hf):
        left, right = project(1, c, hf)
        s1[hf, c, 0] = left
        s1[hf, c, 1] = right
        spread([
            (lambda d, other: s1.at[hf, c, 0, d], rl.at[hf, c, my_half * team + me], L1 + hf, True),
            (lambda d, other: s1.at[hf, c, 1, d], rr.at[hf, c, me], R1 + hf, False),
        ], c)

    def take(c, hf):
        arrive(rl.at[hf, c], L1 + hf, c)
        arrive(rr.at[hf, c], R1 + hf, c)
        unfold([
            (lambda d: rl[hf, c, d], into(ll.at[c, 0], hf)),
            (lambda d: rl[hf, c, team + d], into(ll.at[c, 1], hf)),
            (lambda d: rr[hf, c, d], into(lr.at[c], hf)),
        ])

    def contract(c):
        sums = [
            [
                lax.dot_general(
                    ll[c, h, e], lr[c, e], (((0,), (0,)), ((), ())), preferred_element_type=f32
                )
                for h in range(2)
            ]
            for e in range(each)
        ]

        def piece(hf):
            def pick(e, r, a):
                at = r * first + hf * part + a * depth
                return sums[e][at // LANES][at % LANES:at % LANES + depth]

            def put(d, tile):
                st1[c, d, hf] = tile
            return pick, put

        refold([piece(hf) for hf in range(2)])
        spread([(lambda d, other: st1.at[c, d], rt1.at[c, me], T1, False)], c)

    weight_turn(0)
    for hf in range(2):
        for q in range(depth):
            tile = jnp.concatenate(
                [x_ref[hf * part + a * depth + q] for a in range(fold)], axis=0
            )
            t = hf * span + q * LANES
            xt[:, t:t + LANES] = tile.astype(f32).T
        enter(0, hf)
    for c in range(chunks):
        for hf in range(2):
            left, right = project(0, c, hf)
            if hf == 0:
                sa[c, :, 0] = left
            else:
                sb[c] = left
            sa[c, :, 1 + hf] = right
        if c == 0:
            pl.semaphore_wait(barrier, team)
            pl.semaphore_signal(
                ready, inc=1, device_id=device(0, True), device_id_type=pl.DeviceIdType.MESH
            )
        spread([(lambda d, other: sa.at[c, d], ra.at[c, me], HA, False)], c)
    for c in range(chunks):
        spread([(lambda d, other: sb.at[c, d], rb.at[c, me], HB, False)], c)
    rest_of_setup()
    for hf in range(2):
        open_gate(0, hf)
    for hf in range(2):
        for c in range(chunks):
            multiply(c, hf)
    collect(0)
    for c in range(chunks):
        hand_over(c, 0)
    open_gate(1, 0)
    collect(1)
    for c in range(chunks):
        hand_over(c, 1)
    open_gate(1, 1)
    for c in range(chunks):
        take(c, 0)
    for c in range(chunks):
        take(c, 1)
        contract(c)
    for c in range(chunks):
        arrive(rt1.at[c], T1, c)
        for hf in range(2):
            lay(c, hf, rt1[c, :, hf].astype(f32))
    for hf in range(2):
        leave(1, hf)
    o_ref[...] = xt[...].astype(bf16)

    for c in range(chunks):
        near, both = pl.ds(0, team - 1), pl.ds(0, 2 * team - 1)
        gone(ra.at[c, near], HA, c)
        gone(rb.at[c, near], HB, c)
        for hf in range(2):
            gone(rl.at[hf, c, both], L1 + hf, c)
            gone(rr.at[hf, c, near], R1 + hf, c)
            gone(rt0.at[hf, c, both], T0 + hf, c)
        gone(rt1.at[c, near], T1, c)


def finish(fold, t_ref, o_ref):
    first, second, _ = o_ref.shape
    part = first // 2
    depth = part // fold
    for hf in range(2):
        for q in range(depth):
            t = (hf * depth + q) * LANES
            tile = t_ref[:, t:t + LANES].astype(f32).T.astype(bf16)
            for a in range(fold):
                o_ref[hf * part + a * depth + q] = tile[a * second:(a + 1) * second]


def takes(rows, cols, first, second, channels, hidden):
    if LANES % second or channels != LANES or hidden != LANES or cols % 2 or first % 2:
        return False
    team, fold = rows * (cols // 2), LANES // second
    return (
        cols // 2 == fold and CHUNK % team == 0 and (first // 2) % fold == 0
        and rows * first == cols * second == 2 * LANES
        and first // 2 // fold == 8 and CHUNK // team * 8 == PACK
    )


def solution(mesh):
    rows, cols = mesh.shape["row"], mesh.shape["col"]

    def local(pair_rep, proj_weight, gate_weight, out_weight, in_gain, out_gain):
        first, second, channels = pair_rep.shape
        hidden = out_weight.shape[1]
        args = (pair_rep, proj_weight, gate_weight, out_weight, in_gain, out_gain)
        if not takes(rows, cols, first, second, channels, hidden):
            return plain(*args)
        team = rows * (cols // 2)
        fold = LANES // second
        depth = first // 2 // fold
        chunks = hidden // CHUNK
        each = CHUNK // team
        tile = (each * depth, LANES)
        width = 2 * depth * LANES
        vmem = pl.BlockSpec(memory_space=pltpu.VMEM)
        turned = pl.pallas_call(
            functools.partial(kernel, rows, cols),
            out_shape=jax.ShapeDtypeStruct((channels, width), bf16),
            in_specs=[vmem] * 6,
            out_specs=vmem,
            scratch_shapes=[
                pltpu.VMEM((channels, width), f32),
                pltpu.VMEM((channels, width), bf16),
                pltpu.VMEM((channels, width), f32),
                pltpu.VMEM((hidden, width), f32),
                pltpu.VMEM((2, chunks, 4 * CHUNK, channels), bf16),
                pltpu.VMEM((2, channels, channels), bf16),
                pltpu.VMEM((2, channels, hidden), bf16),
                pltpu.VMEM((fold * LANES, fold * LANES), bf16),
                pltpu.VMEM((2, 2, CHUNK * depth, LANES), f32),
                pltpu.VMEM((CHUNK * depth, LANES), f32),
                pltpu.VMEM((chunks, team, 3) + tile, bf16),
                pltpu.VMEM((chunks, team) + tile, bf16),
                pltpu.VMEM((2, chunks, 2, team) + tile, bf16),
                pltpu.VMEM((chunks, team, 3) + tile, bf16),
                pltpu.VMEM((chunks, team) + tile, bf16),
                pltpu.VMEM((2, chunks, 2 * team) + tile, bf16),
                pltpu.VMEM((2, chunks, team) + tile, bf16),
                pltpu.VMEM((each, LANES, LANES), bf16),
                pltpu.VMEM((chunks, each, 2 * LANES, LANES), bf16),
                pltpu.VMEM((2, chunks, 2, team) + tile, bf16),
                pltpu.VMEM((2, chunks, 2 * team) + tile, bf16),
                pltpu.VMEM((chunks, 2, each, 2 * LANES, LANES), bf16),
                pltpu.VMEM((chunks, each, 2 * LANES, LANES), bf16),
                pltpu.VMEM((chunks, team, 2) + tile, bf16),
                pltpu.VMEM((chunks, team, 2) + tile, bf16),
                pltpu.SemaphoreType.DMA((18, chunks)),
                pltpu.SemaphoreType.REGULAR,
            ],
            compiler_params=pltpu.CompilerParams(collective_id=0, has_side_effects=True),
        )(*args)
        return pl.pallas_call(
            functools.partial(finish, fold),
            out_shape=jax.ShapeDtypeStruct(pair_rep.shape, bf16),
            in_specs=[vmem],
            out_specs=vmem,
        )(turned)

    return jax.shard_map(
        local,
        mesh=mesh,
        in_specs=(P("row", "col", None), P(), P(), P(), P(), P()),
        out_specs=P("row", "col", None),
        check_vma=False,
    )
```

```python
import functools

import jax
import jax.numpy as jnp
from jax import lax
from jax.experimental import pallas as pl
from jax.experimental.pallas import tpu as pltpu
from jax.sharding import PartitionSpec as P

epsilon = 1e-05
LANES = 128
PACK = 16
CHUNK = 32
f32 = jnp.float32
bf16 = jnp.bfloat16


def layer_norm(values, gain_row, reduce_axis):
    center = values - jnp.mean(values, axis=reduce_axis, keepdims=True)
    spread = jnp.mean(center * center, axis=reduce_axis, keepdims=True)
    return center * lax.rsqrt(spread + epsilon) * gain_row


def plain(pair_rep, proj_weight, gate_weight, out_weight, in_gain, out_gain):
    current = pair_rep
    for update_index in range(2):
        widened = current.astype(f32)
        normed = layer_norm(widened, in_gain[update_index], 2).astype(bf16)
        projected = jnp.einsum(
            "ijc,pch->phij", normed, proj_weight[update_index], preferred_element_type=f32
        )
        left_hand = (jax.nn.sigmoid(projected[0]) * projected[1]).astype(bf16)
        right_hand = (jax.nn.sigmoid(projected[2]) * projected[3]).astype(bf16)
        gating = jax.nn.sigmoid(
            jnp.dot(normed, gate_weight[update_index], preferred_element_type=f32)
        )
        left_rows, right_rows = (
            lax.all_to_all(left_hand, "col", split_axis=0, concat_axis=2, tiled=True),
            lax.all_to_all(right_hand, "col", split_axis=0, concat_axis=2, tiled=True),
        )
        if update_index == 0:
            triangle = jnp.einsum(
                "gik,gjk->igj",
                left_rows,
                lax.all_gather(right_rows, "row", axis=1, tiled=True),
                preferred_element_type=f32,
            )
        else:
            left_columns = lax.all_to_all(left_rows, "row", split_axis=2, concat_axis=1, tiled=True)
            triangle = jnp.einsum(
                "gki,gkj->igj",
                left_columns,
                lax.all_gather(right_rows, "row", axis=1, tiled=True),
                preferred_element_type=f32,
            )
        returned = lax.all_to_all(
            triangle.astype(bf16), "col", split_axis=2, concat_axis=1, tiled=True
        )
        mixed_rows = layer_norm(
            returned.astype(f32), out_gain[update_index][None, :, None], 1
        ).astype(bf16)
        update = jnp.einsum(
            "ihj,hc->ijc", mixed_rows, out_weight[update_index], preferred_element_type=f32
        )
        current = (widened + gating * update).astype(bf16)
    return current


def norm_columns(values, gain_column):
    scale = 1.0 / values.shape[0]
    center = values - jnp.sum(values, axis=0, keepdims=True) * scale
    spread = jnp.sum(center * center, axis=0, keepdims=True) * scale
    return center * lax.rsqrt(spread + epsilon) * gain_column


def kernel(rows, cols, x_in, pw_in, gw_in, ow_in, ig_in, og_in, o_ref,
           x_ref, pw_ref, gw_ref, ow_ref, ig_ref, og_ref, loads,
           xt, nt, gt, tt, wt, gwt, owt, perm, shuffle, back,
           sa, sb, s1, ra, rb, rl, rr, ml, mr, st0, rt0, ll, lr, st1, rt1, sems, ready):
    loading = [
        pltpu.make_async_copy(source, target, loads.at[n])
        for n, (source, target) in enumerate((
            (x_in, x_ref), (ig_in, ig_ref), (pw_in, pw_ref),
            (gw_in, gw_ref), (ow_in, ow_ref), (og_in, og_ref),
        ))
    ]
    for load in loading:
        load.start()
    first, second, channels = x_ref.shape
    hidden = ow_ref.shape[1]
    side = cols // 2
    team = rows * side
    fold = LANES // second
    part = first // 2
    depth = part // fold
    block = CHUNK
    chunks = hidden // block
    each = block // team
    high = each * depth
    span = depth * LANES
    width = 2 * span
    step = min(span, 512)
    my_row, my_col = lax.axis_index("row"), lax.axis_index("col")
    my_half, my_side = my_col // side, my_col % side
    me = my_row * side + my_side
    HA, HB, L1, R1, T0, T1 = 0, 1, 2, 4, 6, 8

    def mate(n):
        m = (n * 13) % team if team % 13 else n
        return (my_row + m % rows) % rows, (my_side + m // rows) % side

    def device(n, other):
        row, place = mate(n)
        return row, (1 - my_half if other else my_half) * side + place

    barrier = pltpu.get_barrier_semaphore()

    def greet(n, other):
        pl.semaphore_signal(
            barrier, inc=1, device_id=device(n, other), device_id_type=pl.DeviceIdType.MESH
        )

    greet(0, True)

    @pl.loop(1, team)
    def _(n):
        greet(n, False)

    def send(source, target, kind, slot, n, other):
        row, place = mate(n)
        pltpu.make_async_remote_copy(
            src_ref=source(row * side + place, other),
            dst_ref=target,
            send_sem=sems.at[2 * kind, slot],
            recv_sem=sems.at[2 * kind + 1, slot],
            device_id=device(n, other),
            device_id_type=pl.DeviceIdType.MESH,
        ).start()

    def arrive(buffer, kind, slot):
        pltpu.make_async_copy(buffer, buffer, sems.at[2 * kind + 1, slot]).wait()

    def gone(buffer, kind, slot):
        pltpu.make_async_copy(buffer, buffer, sems.at[2 * kind, slot]).wait()

    def spread(jobs, slot):
        for source, target, kind, across in jobs:
            pltpu.make_async_copy(
                source(me, False), target, sems.at[2 * kind + 1, slot]
            ).start()
            if across:
                send(source, target, kind, slot, 0, True)

        @pl.loop(1, team)
        def _(n):
            for source, target, kind, across in jobs:
                if across:
                    send(source, target, kind, slot, n, True)
                send(source, target, kind, slot, n, False)

    def weight_turn(u):
        for p in range(4):
            turned = pw_ref[u, p].astype(f32).T.astype(bf16)
            for c in range(chunks):
                wt[u, c, p * block:(p + 1) * block, :] = turned[c * block:(c + 1) * block]

    def rest_of_setup():
        for load in loading[3:]:
            load.wait()
        weight_turn(1)
        for u in range(2):
            gwt[u] = gw_ref[u].astype(f32).T.astype(bf16)
            owt[u] = ow_ref[u].astype(f32).T.astype(bf16)
        size = fold * LANES
        bits, low = LANES.bit_length() - 1, second.bit_length() - 1
        to = lax.broadcasted_iota(jnp.int32, (1, size), 1)
        at = lax.broadcasted_iota(jnp.int32, (size, size), 0)
        wanted = (
            (((to & (LANES - 1)) >> low) << bits) + ((to >> bits) << low) + (to & (second - 1))
        )
        perm[...] = jnp.where(at == wanted, 1.0, 0.0).astype(bf16)

    def regroup(parts):
        wide = jnp.concatenate([jnp.concatenate(tiles, axis=1) for tiles in parts], axis=0)
        return jnp.dot(wide, perm[...], preferred_element_type=f32)

    def unfold(sources):
        moved = regroup([
            [get(r * side + p) for p in range(side)] for get, _ in sources for r in range(rows)
        ])
        for s, (_, put) in enumerate(sources):
            for r in range(rows):
                at = (s * rows + r) * high
                for e in range(each):
                    put(e, r, jnp.concatenate([
                        moved[at + e * depth:at + (e + 1) * depth, a * LANES:(a + 1) * LANES]
                        for a in range(fold)
                    ], axis=0).astype(bf16))

    def refold(targets):
        moved = regroup([
            [
                jnp.concatenate([pick(e, r, a) for e in range(each)], axis=0).astype(bf16)
                for a in range(fold)
            ]
            for pick, _ in targets for r in range(rows)
        ])
        for s, (_, put) in enumerate(targets):
            for r in range(rows):
                at = (s * rows + r) * high
                for p in range(side):
                    put(r * side + p, moved[
                        at:at + high, p * LANES:(p + 1) * LANES
                    ].astype(bf16))

    def columns(hf):
        return range(hf * span, (hf + 1) * span, step)

    def gain_of(ref, u):
        return jnp.broadcast_to(ref[u:u + 1, :], (LANES, LANES)).T[:, :1]

    def enter(u, hf):
        gain = gain_of(ig_ref, u)
        for t in columns(hf):
            nt[:, t:t + step] = norm_columns(xt[:, t:t + step], gain).astype(bf16)

    def project(u, c, hf):
        for t in columns(hf):
            got = jnp.dot(wt[u, c], nt[:, t:t + step], preferred_element_type=f32)
            for s in range(2):
                base = 2 * s * block
                hand = jax.nn.sigmoid(got[base:base + block]) * got[base + block:base + 2 * block]
                for k in range(step // LANES):
                    q = (t - hf * span) // LANES + k
                    shuffle[hf, s, pl.ds(q, block, stride=depth), :] = (
                        hand[:, k * LANES:(k + 1) * LANES]
                    )
        return [shuffle[hf, s].reshape(team, high, LANES).astype(bf16) for s in range(2)]

    def open_gate(u, hf):
        for t in columns(hf):
            gt[:, t:t + step] = jax.nn.sigmoid(
                jnp.dot(gwt[u], nt[:, t:t + step], preferred_element_type=f32)
            )

    def lay(c, hf, got):
        back[...] = got.reshape(block * depth, LANES)
        for q in range(depth):
            t = hf * span + q * LANES
            tt[c * block:(c + 1) * block, t:t + LANES] = back[pl.ds(q, block, stride=depth), :]

    def leave(u, hf):
        gain = gain_of(og_ref, u)
        for t in columns(hf):
            mixed = norm_columns(tt[:, t:t + step], gain).astype(bf16)
            update = jnp.dot(owt[u], mixed, preferred_element_type=f32)
            xt[:, t:t + step] = (
                (xt[:, t:t + step] + gt[:, t:t + step] * update).astype(bf16).astype(f32)
            )

    def into(buffer, hf):
        def put(e, r, rows_of):
            at = (hf * rows + r) * part
            buffer[e, at:at + part, :] = rows_of
        return put

    def to_left(e, r, rows_of):
        ml[e, r * part:(r + 1) * part, :] = rows_of

    def to_right(c, hf):
        def put(e, r, rows_of):
            at = r * first + hf * part
            mr[c, e, at:at + part, :] = rows_of
        return put

    def multiply(c, hf):
        if hf == 0:
            arrive(ra.at[c], HA, c)
            unfold([
                (lambda d: ra[c, d, 0], to_left),
                (lambda d: ra[c, d, 1], to_right(c, 0)),
                (lambda d: ra[c, d, 2], to_right(c, 1)),
            ])
        else:
            arrive(rb.at[c], HB, c)
            unfold([(lambda d: rb[c, d], to_left)])
        sums = [
            lax.dot_general(
                ml[e], mr[c, e], (((1,), (1,)), ((), ())), preferred_element_type=f32
            )
            for e in range(each)
        ]

        def piece(h):
            def pick(e, r, a):
                at = (r * fold + a) * depth
                return sums[e][at:at + depth, h * LANES:(h + 1) * LANES]

            def put(d, tile):
                st0[hf, c, h, d] = tile
            return pick, put

        refold([piece(h) for h in range(2)])
        if c == 0 and hf == 0:
            pl.semaphore_wait(ready, 1)
        spread([(
            lambda d, other: st0.at[hf, c, 1 - my_half if other else my_half, d],
            rt0.at[hf, c, my_half * team + me], T0 + hf, True,
        )], c)

    def collect(hf):
        for c in range(chunks):
            arrive(rt0.at[hf, c], T0 + hf, c)
            lay(c, hf, rt0[hf, c, :team].astype(f32) + rt0[hf, c, team:].astype(f32))
        leave(0, hf)
        enter(1, hf)

    def hand_over(c, hf):
        left, right = project(1, c, hf)
        s1[hf, c, 0] = left
        s1[hf, c, 1] = right
        spread([
            (lambda d, other: s1.at[hf, c, 0, d], rl.at[hf, c, my_half * team + me], L1 + hf, True),
            (lambda d, other: s1.at[hf, c, 1, d], rr.at[hf, c, me], R1 + hf, False),
        ], c)

    def take(c, hf):
        arrive(rl.at[hf, c], L1 + hf, c)
        arrive(rr.at[hf, c], R1 + hf, c)
        unfold([
            (lambda d: rl[hf, c, d], into(ll.at[c, 0], hf)),
            (lambda d: rl[hf, c, team + d], into(ll.at[c, 1], hf)),
            (lambda d: rr[hf, c, d], into(lr.at[c], hf)),
        ])

    def contract(c):
        sums = [
            [
                lax.dot_general(
                    ll[c, h, e], lr[c, e], (((0,), (0,)), ((), ())), preferred_element_type=f32
                )
                for h in range(2)
            ]
            for e in range(each)
        ]

        def piece(hf):
            def pick(e, r, a):
                at = r * first + hf * part + a * depth
                return sums[e][at // LANES][at % LANES:at % LANES + depth]

            def put(d, tile):
                st1[c, d, hf] = tile
            return pick, put

        refold([piece(hf) for hf in range(2)])
        spread([(lambda d, other: st1.at[c, d], rt1.at[c, me], T1, False)], c)

    for load in loading[:3]:
        load.wait()
    weight_turn(0)
    for hf in range(2):
        for q in range(depth):
            tile = jnp.concatenate(
                [x_ref[hf * part + a * depth + q] for a in range(fold)], axis=0
            )
            t = hf * span + q * LANES
            xt[:, t:t + LANES] = tile.astype(f32).T
        enter(0, hf)
    for c in range(chunks):
        for hf in range(2):
            left, right = project(0, c, hf)
            if hf == 0:
                sa[c, :, 0] = left
            else:
                sb[c] = left
            sa[c, :, 1 + hf] = right
        if c == 0:
            pl.semaphore_wait(barrier, team)
            pl.semaphore_signal(
                ready, inc=1, device_id=device(0, True), device_id_type=pl.DeviceIdType.MESH
            )
        spread([(lambda d, other: sa.at[c, d], ra.at[c, me], HA, False)], c)
    for c in range(chunks):
        spread([(lambda d, other: sb.at[c, d], rb.at[c, me], HB, False)], c)
    rest_of_setup()
    for hf in range(2):
        open_gate(0, hf)
    for hf in range(2):
        for c in range(chunks):
            multiply(c, hf)
    collect(0)
    for c in range(chunks):
        hand_over(c, 0)
    open_gate(1, 0)
    collect(1)
    for c in range(chunks):
        hand_over(c, 1)
    open_gate(1, 1)
    for c in range(chunks):
        take(c, 0)
    for c in range(chunks):
        take(c, 1)
        contract(c)
    for c in range(chunks):
        arrive(rt1.at[c], T1, c)
        for hf in range(2):
            lay(c, hf, rt1[c, :, hf].astype(f32))
    for hf in range(2):
        leave(1, hf)
    o_ref[...] = xt[...].astype(bf16)

    for c in range(chunks):
        near, both = pl.ds(0, team - 1), pl.ds(0, 2 * team - 1)
        gone(ra.at[c, near], HA, c)
        gone(rb.at[c, near], HB, c)
        for hf in range(2):
            gone(rl.at[hf, c, both], L1 + hf, c)
            gone(rr.at[hf, c, near], R1 + hf, c)
            gone(rt0.at[hf, c, both], T0 + hf, c)
        gone(rt1.at[c, near], T1, c)


def finish(fold, t_ref, o_ref):
    first, second, _ = o_ref.shape
    part = first // 2
    depth = part // fold
    for hf in range(2):
        for q in range(depth):
            t = (hf * depth + q) * LANES
            tile = t_ref[:, t:t + LANES].astype(f32).T.astype(bf16)
            for a in range(fold):
                o_ref[hf * part + a * depth + q] = tile[a * second:(a + 1) * second]


def takes(rows, cols, first, second, channels, hidden):
    if LANES % second or channels != LANES or hidden != LANES or cols % 2 or first % 2:
        return False
    team, fold = rows * (cols // 2), LANES // second
    return (
        cols // 2 == fold and CHUNK % team == 0 and (first // 2) % fold == 0
        and rows * first == cols * second == 2 * LANES
        and first // 2 // fold == 8 and CHUNK // team * 8 == PACK
    )


def solution(mesh):
    rows, cols = mesh.shape["row"], mesh.shape["col"]

    def local(pair_rep, proj_weight, gate_weight, out_weight, in_gain, out_gain):
        first, second, channels = pair_rep.shape
        hidden = out_weight.shape[1]
        args = (pair_rep, proj_weight, gate_weight, out_weight, in_gain, out_gain)
        if not takes(rows, cols, first, second, channels, hidden):
            return plain(*args)
        team = rows * (cols // 2)
        fold = LANES // second
        depth = first // 2 // fold
        chunks = hidden // CHUNK
        each = CHUNK // team
        tile = (each * depth, LANES)
        width = 2 * depth * LANES
        vmem = pl.BlockSpec(memory_space=pltpu.VMEM)
        turned = pl.pallas_call(
            functools.partial(kernel, rows, cols),
            out_shape=pltpu.VMEM((channels, width), bf16),
            in_specs=[pl.BlockSpec(memory_space=pl.ANY)] * 6,
            out_specs=vmem,
            scratch_shapes=[
                *(pltpu.VMEM(arg.shape, arg.dtype) for arg in args),
                pltpu.SemaphoreType.DMA((len(args),)),
                pltpu.VMEM((channels, width), f32),
                pltpu.VMEM((channels, width), bf16),
                pltpu.VMEM((channels, width), f32),
                pltpu.VMEM((hidden, width), f32),
                pltpu.VMEM((2, chunks, 4 * CHUNK, channels), bf16),
                pltpu.VMEM((2, channels, channels), bf16),
                pltpu.VMEM((2, channels, hidden), bf16),
                pltpu.VMEM((fold * LANES, fold * LANES), bf16),
                pltpu.VMEM((2, 2, CHUNK * depth, LANES), f32),
                pltpu.VMEM((CHUNK * depth, LANES), f32),
                pltpu.VMEM((chunks, team, 3) + tile, bf16),
                pltpu.VMEM((chunks, team) + tile, bf16),
                pltpu.VMEM((2, chunks, 2, team) + tile, bf16),
                pltpu.VMEM((chunks, team, 3) + tile, bf16),
                pltpu.VMEM((chunks, team) + tile, bf16),
                pltpu.VMEM((2, chunks, 2 * team) + tile, bf16),
                pltpu.VMEM((2, chunks, team) + tile, bf16),
                pltpu.VMEM((each, LANES, LANES), bf16),
                pltpu.VMEM((chunks, each, 2 * LANES, LANES), bf16),
                pltpu.VMEM((2, chunks, 2, team) + tile, bf16),
                pltpu.VMEM((2, chunks, 2 * team) + tile, bf16),
                pltpu.VMEM((chunks, 2, each, 2 * LANES, LANES), bf16),
                pltpu.VMEM((chunks, each, 2 * LANES, LANES), bf16),
                pltpu.VMEM((chunks, team, 2) + tile, bf16),
                pltpu.VMEM((chunks, team, 2) + tile, bf16),
                pltpu.SemaphoreType.DMA((18, chunks)),
                pltpu.SemaphoreType.REGULAR,
            ],
            compiler_params=pltpu.CompilerParams(
                collective_id=0, has_side_effects=True, vmem_limit_bytes=62 * 2 ** 20
            ),
        )(*args)
        return pl.pallas_call(
            functools.partial(finish, fold),
            out_shape=jax.ShapeDtypeStruct(pair_rep.shape, bf16),
            in_specs=[vmem],
            out_specs=vmem,
            compiler_params=pltpu.CompilerParams(vmem_limit_bytes=4 * 2 ** 20),
        )(turned)

    return jax.shard_map(
        local,
        mesh=mesh,
        in_specs=(P("row", "col", None), P(), P(), P(), P(), P()),
        out_specs=P("row", "col", None),
        check_vma=False,
    )
```

```python
import functools

import jax
import jax.numpy as jnp
from jax import lax
from jax.experimental import pallas as pl
from jax.experimental.pallas import tpu as pltpu
from jax.sharding import PartitionSpec as P

epsilon = 1e-05
LANES = 128
PACK = 16
CHUNK = 32
f32 = jnp.float32
bf16 = jnp.bfloat16


def layer_norm(values, gain_row, reduce_axis):
    center = values - jnp.mean(values, axis=reduce_axis, keepdims=True)
    spread = jnp.mean(center * center, axis=reduce_axis, keepdims=True)
    return center * lax.rsqrt(spread + epsilon) * gain_row


def plain(pair_rep, proj_weight, gate_weight, out_weight, in_gain, out_gain):
    current = pair_rep
    for update_index in range(2):
        widened = current.astype(f32)
        normed = layer_norm(widened, in_gain[update_index], 2).astype(bf16)
        projected = jnp.einsum(
            "ijc,pch->phij", normed, proj_weight[update_index], preferred_element_type=f32
        )
        left_hand = (jax.nn.sigmoid(projected[0]) * projected[1]).astype(bf16)
        right_hand = (jax.nn.sigmoid(projected[2]) * projected[3]).astype(bf16)
        gating = jax.nn.sigmoid(
            jnp.dot(normed, gate_weight[update_index], preferred_element_type=f32)
        )
        left_rows, right_rows = (
            lax.all_to_all(left_hand, "col", split_axis=0, concat_axis=2, tiled=True),
            lax.all_to_all(right_hand, "col", split_axis=0, concat_axis=2, tiled=True),
        )
        if update_index == 0:
            triangle = jnp.einsum(
                "gik,gjk->igj",
                left_rows,
                lax.all_gather(right_rows, "row", axis=1, tiled=True),
                preferred_element_type=f32,
            )
        else:
            left_columns = lax.all_to_all(left_rows, "row", split_axis=2, concat_axis=1, tiled=True)
            triangle = jnp.einsum(
                "gki,gkj->igj",
                left_columns,
                lax.all_gather(right_rows, "row", axis=1, tiled=True),
                preferred_element_type=f32,
            )
        returned = lax.all_to_all(
            triangle.astype(bf16), "col", split_axis=2, concat_axis=1, tiled=True
        )
        mixed_rows = layer_norm(
            returned.astype(f32), out_gain[update_index][None, :, None], 1
        ).astype(bf16)
        update = jnp.einsum(
            "ihj,hc->ijc", mixed_rows, out_weight[update_index], preferred_element_type=f32
        )
        current = (widened + gating * update).astype(bf16)
    return current


def norm_columns(values, gain_column):
    scale = 1.0 / values.shape[0]
    center = values - jnp.sum(values, axis=0, keepdims=True) * scale
    spread = jnp.sum(center * center, axis=0, keepdims=True) * scale
    return center * lax.rsqrt(spread + epsilon) * gain_column


def kernel(rows, cols, x_in, pw_in, gw_in, ow_in, ig_in, og_in, o_ref,
           x_ref, pw_ref, gw_ref, ow_ref, ig_ref, og_ref, loads,
           xt, nt, gt, tt, wt, gwt, owt, perm, shuffle, back,
           sa, sb, s1, ra, rb, rl, rr, ml, mr, st0, rt0, ll, lr, st1, rt1, sems, ready):
    loading = [
        pltpu.make_async_copy(source, target, loads.at[n])
        for n, (source, target) in enumerate((
            (x_in, x_ref), (ig_in, ig_ref), (pw_in, pw_ref),
            (gw_in, gw_ref), (ow_in, ow_ref), (og_in, og_ref),
        ))
    ]
    for load in loading:
        load.start()
    first, second, channels = x_ref.shape
    hidden = ow_ref.shape[1]
    side = cols // 2
    team = rows * side
    fold = LANES // second
    part = first // 2
    depth = part // fold
    block = CHUNK
    chunks = hidden // block
    each = block // team
    high = each * depth
    span = depth * LANES
    width = 2 * span
    step = min(span, 512)
    my_row, my_col = lax.axis_index("row"), lax.axis_index("col")
    my_half, my_side = my_col // side, my_col % side
    me = my_row * side + my_side
    HA, HB, L1, R1, T0, T1 = 0, 1, 2, 4, 6, 8

    def mate(n):
        m = (n * 13) % team if team % 13 else n
        return (my_row + m % rows) % rows, (my_side + m // rows) % side

    def device(n, other):
        row, place = mate(n)
        return row, (1 - my_half if other else my_half) * side + place

    barrier = pltpu.get_barrier_semaphore()

    def greet(n, other):
        pl.semaphore_signal(
            barrier, inc=1, device_id=device(n, other), device_id_type=pl.DeviceIdType.MESH
        )

    greet(0, True)

    @pl.loop(1, team)
    def _(n):
        greet(n, False)

    def send(source, target, kind, slot, n, other):
        row, place = mate(n)
        pltpu.make_async_remote_copy(
            src_ref=source(row * side + place, other),
            dst_ref=target,
            send_sem=sems.at[2 * kind, slot],
            recv_sem=sems.at[2 * kind + 1, slot],
            device_id=device(n, other),
            device_id_type=pl.DeviceIdType.MESH,
        ).start()

    def arrive(buffer, kind, slot):
        pltpu.make_async_copy(buffer, buffer, sems.at[2 * kind + 1, slot]).wait()

    def gone(buffer, kind, slot):
        pltpu.make_async_copy(buffer, buffer, sems.at[2 * kind, slot]).wait()

    def spread(jobs, slot):
        for source, target, kind, across in jobs:
            pltpu.make_async_copy(
                source(me, False), target, sems.at[2 * kind + 1, slot]
            ).start()
            if across:
                send(source, target, kind, slot, 0, True)

        for n in range(1, team):
            for source, target, kind, across in jobs:
                if across:
                    send(source, target, kind, slot, n, True)
                send(source, target, kind, slot, n, False)

    def weight_turn(u):
        for p in range(4):
            turned = pw_ref[u, p].astype(f32).T.astype(bf16)
            for c in range(chunks):
                wt[u, c, p * block:(p + 1) * block, :] = turned[c * block:(c + 1) * block]

    def rest_of_setup():
        for load in loading[3:]:
            load.wait()
        weight_turn(1)
        for u in range(2):
            gwt[u] = gw_ref[u].astype(f32).T.astype(bf16)
            owt[u] = ow_ref[u].astype(f32).T.astype(bf16)
        size = fold * LANES
        bits, low = LANES.bit_length() - 1, second.bit_length() - 1
        to = lax.broadcasted_iota(jnp.int32, (1, size), 1)
        at = lax.broadcasted_iota(jnp.int32, (size, size), 0)
        wanted = (
            (((to & (LANES - 1)) >> low) << bits) + ((to >> bits) << low) + (to & (second - 1))
        )
        perm[...] = jnp.where(at == wanted, 1.0, 0.0).astype(bf16)

    def regroup(parts):
        wide = jnp.concatenate([jnp.concatenate(tiles, axis=1) for tiles in parts], axis=0)
        return jnp.dot(wide, perm[...], preferred_element_type=f32)

    def unfold(sources):
        moved = regroup([
            [get(r * side + p) for p in range(side)] for get, _ in sources for r in range(rows)
        ])
        for s, (_, put) in enumerate(sources):
            for r in range(rows):
                at = (s * rows + r) * high
                for e in range(each):
                    put(e, r, jnp.concatenate([
                        moved[at + e * depth:at + (e + 1) * depth, a * LANES:(a + 1) * LANES]
                        for a in range(fold)
                    ], axis=0).astype(bf16))

    def refold(targets):
        moved = regroup([
            [
                jnp.concatenate([pick(e, r, a) for e in range(each)], axis=0).astype(bf16)
                for a in range(fold)
            ]
            for pick, _ in targets for r in range(rows)
        ])
        for s, (_, put) in enumerate(targets):
            for r in range(rows):
                at = (s * rows + r) * high
                for p in range(side):
                    put(r * side + p, moved[
                        at:at + high, p * LANES:(p + 1) * LANES
                    ].astype(bf16))

    def columns(hf):
        return range(hf * span, (hf + 1) * span, step)

    def gain_of(ref, u):
        return jnp.broadcast_to(ref[u:u + 1, :], (LANES, LANES)).T[:, :1]

    def enter(u, hf):
        gain = gain_of(ig_ref, u)
        for t in columns(hf):
            nt[:, t:t + step] = norm_columns(xt[:, t:t + step], gain).astype(bf16)

    def project(u, c, hf):
        for t in columns(hf):
            got = jnp.dot(wt[u, c], nt[:, t:t + step], preferred_element_type=f32)
            for s in range(2):
                base = 2 * s * block
                hand = jax.nn.sigmoid(got[base:base + block]) * got[base + block:base + 2 * block]
                for k in range(step // LANES):
                    q = (t - hf * span) // LANES + k
                    shuffle[hf, s, pl.ds(q, block, stride=depth), :] = (
                        hand[:, k * LANES:(k + 1) * LANES]
                    )
        return [shuffle[hf, s].reshape(team, high, LANES).astype(bf16) for s in range(2)]

    def open_gate(u, hf):
        for t in columns(hf):
            gt[:, t:t + step] = jax.nn.sigmoid(
                jnp.dot(gwt[u], nt[:, t:t + step], preferred_element_type=f32)
            )

    def lay(c, hf, got):
        back[...] = got.reshape(block * depth, LANES)
        for q in range(depth):
            t = hf * span + q * LANES
            tt[c * block:(c + 1) * block, t:t + LANES] = back[pl.ds(q, block, stride=depth), :]

    def leave(u, hf):
        gain = gain_of(og_ref, u)
        for t in columns(hf):
            mixed = norm_columns(tt[:, t:t + step], gain).astype(bf16)
            update = jnp.dot(owt[u], mixed, preferred_element_type=f32)
            xt[:, t:t + step] = (
                (xt[:, t:t + step] + gt[:, t:t + step] * update).astype(bf16).astype(f32)
            )

    def into(buffer, hf):
        def put(e, r, rows_of):
            at = (hf * rows + r) * part
            buffer[e, at:at + part, :] = rows_of
        return put

    def to_left(e, r, rows_of):
        ml[e, r * part:(r + 1) * part, :] = rows_of

    def to_right(c, hf):
        def put(e, r, rows_of):
            at = r * first + hf * part
            mr[c, e, at:at + part, :] = rows_of
        return put

    def multiply(c, hf):
        if hf == 0:
            arrive(ra.at[c], HA, c)
            unfold([
                (lambda d: ra[c, d, 0], to_left),
                (lambda d: ra[c, d, 1], to_right(c, 0)),
                (lambda d: ra[c, d, 2], to_right(c, 1)),
            ])
        else:
            arrive(rb.at[c], HB, c)
            unfold([(lambda d: rb[c, d], to_left)])
        sums = [
            lax.dot_general(
                ml[e], mr[c, e], (((1,), (1,)), ((), ())), preferred_element_type=f32
            )
            for e in range(each)
        ]

        def piece(h):
            def pick(e, r, a):
                at = (r * fold + a) * depth
                return sums[e][at:at + depth, h * LANES:(h + 1) * LANES]

            def put(d, tile):
                st0[hf, c, h, d] = tile
            return pick, put

        refold([piece(h) for h in range(2)])
        if c == 0 and hf == 0:
            pl.semaphore_wait(ready, 1)
        spread([(
            lambda d, other: st0.at[hf, c, 1 - my_half if other else my_half, d],
            rt0.at[hf, c, my_half * team + me], T0 + hf, True,
        )], c)

    def collect(hf):
        for c in range(chunks):
            arrive(rt0.at[hf, c], T0 + hf, c)
            lay(c, hf, rt0[hf, c, :team].astype(f32) + rt0[hf, c, team:].astype(f32))
        leave(0, hf)
        enter(1, hf)

    def hand_over(c, hf):
        left, right = project(1, c, hf)
        s1[hf, c, 0] = left
        s1[hf, c, 1] = right
        spread([
            (lambda d, other: s1.at[hf, c, 0, d], rl.at[hf, c, my_half * team + me], L1 + hf, True),
            (lambda d, other: s1.at[hf, c, 1, d], rr.at[hf, c, me], R1 + hf, False),
        ], c)

    def take(c, hf):
        arrive(rl.at[hf, c], L1 + hf, c)
        arrive(rr.at[hf, c], R1 + hf, c)
        unfold([
            (lambda d: rl[hf, c, d], into(ll.at[c, 0], hf)),
            (lambda d: rl[hf, c, team + d], into(ll.at[c, 1], hf)),
            (lambda d: rr[hf, c, d], into(lr.at[c], hf)),
        ])

    def contract(c):
        sums = [
            [
                lax.dot_general(
                    ll[c, h, e], lr[c, e], (((0,), (0,)), ((), ())), preferred_element_type=f32
                )
                for h in range(2)
            ]
            for e in range(each)
        ]

        def piece(hf):
            def pick(e, r, a):
                at = r * first + hf * part + a * depth
                return sums[e][at // LANES][at % LANES:at % LANES + depth]

            def put(d, tile):
                st1[c, d, hf] = tile
            return pick, put

        refold([piece(hf) for hf in range(2)])
        spread([(lambda d, other: st1.at[c, d], rt1.at[c, me], T1, False)], c)

    for load in loading[:3]:
        load.wait()
    weight_turn(0)
    for hf in range(2):
        for q in range(depth):
            tile = jnp.concatenate(
                [x_ref[hf * part + a * depth + q] for a in range(fold)], axis=0
            )
            t = hf * span + q * LANES
            xt[:, t:t + LANES] = tile.astype(f32).T
        enter(0, hf)
    for c in range(chunks):
        for hf in range(2):
            left, right = project(0, c, hf)
            if hf == 0:
                sa[c, :, 0] = left
            else:
                sb[c] = left
            sa[c, :, 1 + hf] = right
        if c == 0:
            pl.semaphore_wait(barrier, team)
            pl.semaphore_signal(
                ready, inc=1, device_id=device(0, True), device_id_type=pl.DeviceIdType.MESH
            )
        spread([(lambda d, other: sa.at[c, d], ra.at[c, me], HA, False)], c)
    rest_of_setup()
    for c in range(1):
        multiply(c, 0)
    for c in range(chunks):
        spread([(lambda d, other: sb.at[c, d], rb.at[c, me], HB, False)], c)
    for hf in range(2):
        open_gate(0, hf)
    for c in range(1, chunks):
        multiply(c, 0)
    for c in range(chunks):
        multiply(c, 1)
    collect(0)
    for c in range(chunks):
        hand_over(c, 0)
    open_gate(1, 0)
    collect(1)
    for c in range(chunks):
        hand_over(c, 1)
    open_gate(1, 1)
    for c in range(chunks):
        take(c, 0)
    for c in range(chunks):
        take(c, 1)
        contract(c)
    for c in range(chunks):
        arrive(rt1.at[c], T1, c)
        for hf in range(2):
            lay(c, hf, rt1[c, :, hf].astype(f32))
    for hf in range(2):
        leave(1, hf)
    o_ref[...] = xt[...].astype(bf16)

    for c in range(chunks):
        near, both = pl.ds(0, team - 1), pl.ds(0, 2 * team - 1)
        gone(ra.at[c, near], HA, c)
        gone(rb.at[c, near], HB, c)
        for hf in range(2):
            gone(rl.at[hf, c, both], L1 + hf, c)
            gone(rr.at[hf, c, near], R1 + hf, c)
            gone(rt0.at[hf, c, both], T0 + hf, c)
        gone(rt1.at[c, near], T1, c)


def finish(fold, t_ref, o_ref):
    first, second, _ = o_ref.shape
    part = first // 2
    depth = part // fold
    for hf in range(2):
        for q in range(depth):
            t = (hf * depth + q) * LANES
            tile = t_ref[:, t:t + LANES].astype(f32).T.astype(bf16)
            for a in range(fold):
                o_ref[hf * part + a * depth + q] = tile[a * second:(a + 1) * second]


def takes(rows, cols, first, second, channels, hidden):
    if LANES % second or channels != LANES or hidden != LANES or cols % 2 or first % 2:
        return False
    team, fold = rows * (cols // 2), LANES // second
    return (
        cols // 2 == fold and CHUNK % team == 0 and (first // 2) % fold == 0
        and rows * first == cols * second == 2 * LANES
        and first // 2 // fold == 8 and CHUNK // team * 8 == PACK
    )


def solution(mesh):
    rows, cols = mesh.shape["row"], mesh.shape["col"]

    def local(pair_rep, proj_weight, gate_weight, out_weight, in_gain, out_gain):
        first, second, channels = pair_rep.shape
        hidden = out_weight.shape[1]
        args = (pair_rep, proj_weight, gate_weight, out_weight, in_gain, out_gain)
        if not takes(rows, cols, first, second, channels, hidden):
            return plain(*args)
        team = rows * (cols // 2)
        fold = LANES // second
        depth = first // 2 // fold
        chunks = hidden // CHUNK
        each = CHUNK // team
        tile = (each * depth, LANES)
        width = 2 * depth * LANES
        vmem = pl.BlockSpec(memory_space=pltpu.VMEM)
        turned = pl.pallas_call(
            functools.partial(kernel, rows, cols),
            out_shape=pltpu.VMEM((channels, width), bf16),
            in_specs=[pl.BlockSpec(memory_space=pl.ANY)] * 6,
            out_specs=vmem,
            scratch_shapes=[
                *(pltpu.VMEM(arg.shape, arg.dtype) for arg in args),
                pltpu.SemaphoreType.DMA((len(args),)),
                pltpu.VMEM((channels, width), f32),
                pltpu.VMEM((channels, width), bf16),
                pltpu.VMEM((channels, width), f32),
                pltpu.VMEM((hidden, width), f32),
                pltpu.VMEM((2, chunks, 4 * CHUNK, channels), bf16),
                pltpu.VMEM((2, channels, channels), bf16),
                pltpu.VMEM((2, channels, hidden), bf16),
                pltpu.VMEM((fold * LANES, fold * LANES), bf16),
                pltpu.VMEM((2, 2, CHUNK * depth, LANES), f32),
                pltpu.VMEM((CHUNK * depth, LANES), f32),
                pltpu.VMEM((chunks, team, 3) + tile, bf16),
                pltpu.VMEM((chunks, team) + tile, bf16),
                pltpu.VMEM((2, chunks, 2, team) + tile, bf16),
                pltpu.VMEM((chunks, team, 3) + tile, bf16),
                pltpu.VMEM((chunks, team) + tile, bf16),
                pltpu.VMEM((2, chunks, 2 * team) + tile, bf16),
                pltpu.VMEM((2, chunks, team) + tile, bf16),
                pltpu.VMEM((each, LANES, LANES), bf16),
                pltpu.VMEM((chunks, each, 2 * LANES, LANES), bf16),
                pltpu.VMEM((2, chunks, 2, team) + tile, bf16),
                pltpu.VMEM((2, chunks, 2 * team) + tile, bf16),
                pltpu.VMEM((chunks, 2, each, 2 * LANES, LANES), bf16),
                pltpu.VMEM((chunks, each, 2 * LANES, LANES), bf16),
                pltpu.VMEM((chunks, team, 2) + tile, bf16),
                pltpu.VMEM((chunks, team, 2) + tile, bf16),
                pltpu.SemaphoreType.DMA((18, chunks)),
                pltpu.SemaphoreType.REGULAR,
            ],
            compiler_params=pltpu.CompilerParams(
                collective_id=0, has_side_effects=True, vmem_limit_bytes=62 * 2 ** 20
            ),
        )(*args)
        return pl.pallas_call(
            functools.partial(finish, fold),
            out_shape=jax.ShapeDtypeStruct(pair_rep.shape, bf16),
            in_specs=[vmem],
            out_specs=vmem,
            compiler_params=pltpu.CompilerParams(vmem_limit_bytes=4 * 2 ** 20),
        )(turned)

    return jax.shard_map(
        local,
        mesh=mesh,
        in_specs=(P("row", "col", None), P(), P(), P(), P(), P()),
        out_specs=P("row", "col", None),
        check_vma=False,
    )
```

```python
import functools

import jax
import jax.numpy as jnp
from jax import lax
from jax.experimental import pallas as pl
from jax.experimental.pallas import tpu as pltpu
from jax.sharding import PartitionSpec as P

epsilon = 1e-05
LANES = 128
PACK = 16
CHUNK = 32
f32 = jnp.float32
bf16 = jnp.bfloat16


def layer_norm(values, gain_row, reduce_axis):
    center = values - jnp.mean(values, axis=reduce_axis, keepdims=True)
    spread = jnp.mean(center * center, axis=reduce_axis, keepdims=True)
    return center * lax.rsqrt(spread + epsilon) * gain_row


def plain(pair_rep, proj_weight, gate_weight, out_weight, in_gain, out_gain):
    current = pair_rep
    for update_index in range(2):
        widened = current.astype(f32)
        normed = layer_norm(widened, in_gain[update_index], 2).astype(bf16)
        projected = jnp.einsum(
            "ijc,pch->phij", normed, proj_weight[update_index], preferred_element_type=f32
        )
        left_hand = (jax.nn.sigmoid(projected[0]) * projected[1]).astype(bf16)
        right_hand = (jax.nn.sigmoid(projected[2]) * projected[3]).astype(bf16)
        gating = jax.nn.sigmoid(
            jnp.dot(normed, gate_weight[update_index], preferred_element_type=f32)
        )
        left_rows, right_rows = (
            lax.all_to_all(left_hand, "col", split_axis=0, concat_axis=2, tiled=True),
            lax.all_to_all(right_hand, "col", split_axis=0, concat_axis=2, tiled=True),
        )
        if update_index == 0:
            triangle = jnp.einsum(
                "gik,gjk->igj",
                left_rows,
                lax.all_gather(right_rows, "row", axis=1, tiled=True),
                preferred_element_type=f32,
            )
        else:
            left_columns = lax.all_to_all(left_rows, "row", split_axis=2, concat_axis=1, tiled=True)
            triangle = jnp.einsum(
                "gki,gkj->igj",
                left_columns,
                lax.all_gather(right_rows, "row", axis=1, tiled=True),
                preferred_element_type=f32,
            )
        returned = lax.all_to_all(
            triangle.astype(bf16), "col", split_axis=2, concat_axis=1, tiled=True
        )
        mixed_rows = layer_norm(
            returned.astype(f32), out_gain[update_index][None, :, None], 1
        ).astype(bf16)
        update = jnp.einsum(
            "ihj,hc->ijc", mixed_rows, out_weight[update_index], preferred_element_type=f32
        )
        current = (widened + gating * update).astype(bf16)
    return current


def norm_columns(values, gain_column):
    scale = 1.0 / values.shape[0]
    center = values - jnp.sum(values, axis=0, keepdims=True) * scale
    spread = jnp.sum(center * center, axis=0, keepdims=True) * scale
    return center * lax.rsqrt(spread + epsilon) * gain_column


def kernel(rows, cols, x_in, pw_in, gw_in, ow_in, ig_in, og_in, o_ref,
           x_ref, pw_ref, gw_ref, ow_ref, ig_ref, og_ref, loads,
           xt, nt, gt, tt, wt, gwt, owt, perm, shuffle, back,
           sa, sb, s1, ra, rb, rl, rr, ml, mr, st0, rt0, ll, lr, st1, rt1, sems, ready):
    loading = [
        pltpu.make_async_copy(source, target, loads.at[n])
        for n, (source, target) in enumerate((
            (x_in, x_ref), (ig_in, ig_ref), (pw_in.at[0], pw_ref.at[0]),
            (pw_in.at[1], pw_ref.at[1]), (gw_in, gw_ref), (ow_in, ow_ref), (og_in, og_ref),
        ))
    ]
    for load in loading:
        load.start()
    first, second, channels = x_ref.shape
    hidden = ow_ref.shape[1]
    side = cols // 2
    team = rows * side
    fold = LANES // second
    part = first // 2
    depth = part // fold
    block = CHUNK
    chunks = hidden // block
    each = block // team
    high = each * depth
    span = depth * LANES
    width = 2 * span
    step = min(span, 512)
    my_row, my_col = lax.axis_index("row"), lax.axis_index("col")
    my_half, my_side = my_col // side, my_col % side
    me = my_row * side + my_side
    HA, HB, L1, R1, T0, T1 = 0, 1, 2, 4, 6, 8

    def mate(n):
        m = (n * 13) % team if team % 13 else n
        return (my_row + m % rows) % rows, (my_side + m // rows) % side

    def device(n, other):
        row, place = mate(n)
        return row, (1 - my_half if other else my_half) * side + place

    barrier = pltpu.get_barrier_semaphore()

    def greet(n, other):
        pl.semaphore_signal(
            barrier, inc=1, device_id=device(n, other), device_id_type=pl.DeviceIdType.MESH
        )

    greet(0, True)

    @pl.loop(1, team)
    def _(n):
        greet(n, False)

    def send(source, target, kind, slot, n, other):
        row, place = mate(n)
        pltpu.make_async_remote_copy(
            src_ref=source(row * side + place, other),
            dst_ref=target,
            send_sem=sems.at[2 * kind, slot],
            recv_sem=sems.at[2 * kind + 1, slot],
            device_id=device(n, other),
            device_id_type=pl.DeviceIdType.MESH,
        ).start()

    def arrive(buffer, kind, slot):
        pltpu.make_async_copy(buffer, buffer, sems.at[2 * kind + 1, slot]).wait()

    def gone(buffer, kind, slot):
        pltpu.make_async_copy(buffer, buffer, sems.at[2 * kind, slot]).wait()

    def spread(jobs, slot):
        for source, target, kind, across in jobs:
            pltpu.make_async_copy(
                source(me, False), target, sems.at[2 * kind + 1, slot]
            ).start()
            if across:
                send(source, target, kind, slot, 0, True)

        for n in range(1, team):
            for source, target, kind, across in jobs:
                if across:
                    send(source, target, kind, slot, n, True)
                send(source, target, kind, slot, n, False)

    def weight_turn(u):
        for p in range(4):
            turned = pw_ref[u, p].astype(f32).T.astype(bf16)
            for c in range(chunks):
                wt[u, c, p * block:(p + 1) * block, :] = turned[c * block:(c + 1) * block]

    def rest_of_setup():
        for load in loading[3:]:
            load.wait()
        weight_turn(1)
        for u in range(2):
            gwt[u] = gw_ref[u].astype(f32).T.astype(bf16)
            owt[u] = ow_ref[u].astype(f32).T.astype(bf16)
        size = fold * LANES
        bits, low = LANES.bit_length() - 1, second.bit_length() - 1
        to = lax.broadcasted_iota(jnp.int32, (1, size), 1)
        at = lax.broadcasted_iota(jnp.int32, (size, size), 0)
        wanted = (
            (((to & (LANES - 1)) >> low) << bits) + ((to >> bits) << low) + (to & (second - 1))
        )
        perm[...] = jnp.where(at == wanted, 1.0, 0.0).astype(bf16)

    def regroup(parts):
        wide = jnp.concatenate([jnp.concatenate(tiles, axis=1) for tiles in parts], axis=0)
        return jnp.dot(wide, perm[...], preferred_element_type=f32)

    def unfold(sources):
        moved = regroup([
            [get(r * side + p) for p in range(side)] for get, _ in sources for r in range(rows)
        ])
        for s, (_, put) in enumerate(sources):
            for r in range(rows):
                at = (s * rows + r) * high
                for e in range(each):
                    put(e, r, jnp.concatenate([
                        moved[at + e * depth:at + (e + 1) * depth, a * LANES:(a + 1) * LANES]
                        for a in range(fold)
                    ], axis=0).astype(bf16))

    def refold(targets):
        moved = regroup([
            [
                jnp.concatenate([pick(e, r, a) for e in range(each)], axis=0).astype(bf16)
                for a in range(fold)
            ]
            for pick, _ in targets for r in range(rows)
        ])
        for s, (_, put) in enumerate(targets):
            for r in range(rows):
                at = (s * rows + r) * high
                for p in range(side):
                    put(r * side + p, moved[
                        at:at + high, p * LANES:(p + 1) * LANES
                    ].astype(bf16))

    def columns(hf):
        return range(hf * span, (hf + 1) * span, step)

    def gain_of(ref, u):
        return jnp.broadcast_to(ref[u:u + 1, :], (LANES, LANES)).T[:, :1]

    def enter(u, hf):
        gain = gain_of(ig_ref, u)
        for t in columns(hf):
            nt[:, t:t + step] = norm_columns(xt[:, t:t + step], gain).astype(bf16)

    def project(u, c, hf):
        for t in columns(hf):
            got = jnp.dot(wt[u, c], nt[:, t:t + step], preferred_element_type=f32)
            for s in range(2):
                base = 2 * s * block
                hand = jax.nn.sigmoid(got[base:base + block]) * got[base + block:base + 2 * block]
                for k in range(step // LANES):
                    q = (t - hf * span) // LANES + k
                    shuffle[hf, s, pl.ds(q, block, stride=depth), :] = (
                        hand[:, k * LANES:(k + 1) * LANES]
                    )
        return [shuffle[hf, s].reshape(team, high, LANES).astype(bf16) for s in range(2)]

    def open_gate(u, hf):
        for t in columns(hf):
            gt[:, t:t + step] = jax.nn.sigmoid(
                jnp.dot(gwt[u], nt[:, t:t + step], preferred_element_type=f32)
            )

    def lay(c, hf, got):
        back[...] = got.reshape(block * depth, LANES)
        for q in range(depth):
            t = hf * span + q * LANES
            tt[c * block:(c + 1) * block, t:t + LANES] = back[pl.ds(q, block, stride=depth), :]

    def leave(u, hf):
        gain = gain_of(og_ref, u)
        for t in columns(hf):
            mixed = norm_columns(tt[:, t:t + step], gain).astype(bf16)
            update = jnp.dot(owt[u], mixed, preferred_element_type=f32)
            xt[:, t:t + step] = (
                (xt[:, t:t + step] + gt[:, t:t + step] * update).astype(bf16).astype(f32)
            )

    def into(buffer, hf):
        def put(e, r, rows_of):
            at = (hf * rows + r) * part
            buffer[e, at:at + part, :] = rows_of
        return put

    def to_left(e, r, rows_of):
        ml[e, r * part:(r + 1) * part, :] = rows_of

    def to_right(c, hf):
        def put(e, r, rows_of):
            at = r * first + hf * part
            mr[c, e, at:at + part, :] = rows_of
        return put

    def multiply(c, hf):
        if hf == 0:
            arrive(ra.at[c], HA, c)
            unfold([
                (lambda d: ra[c, d, 0], to_left),
                (lambda d: ra[c, d, 1], to_right(c, 0)),
                (lambda d: ra[c, d, 2], to_right(c, 1)),
            ])
        else:
            arrive(rb.at[c], HB, c)
            unfold([(lambda d: rb[c, d], to_left)])
        sums = [
            lax.dot_general(
                ml[e], mr[c, e], (((1,), (1,)), ((), ())), preferred_element_type=f32
            )
            for e in range(each)
        ]

        def piece(h):
            def pick(e, r, a):
                at = (r * fold + a) * depth
                return sums[e][at:at + depth, h * LANES:(h + 1) * LANES]

            def put(d, tile):
                st0[hf, c, h, d] = tile
            return pick, put

        refold([piece(h) for h in range(2)])
        if c == 0 and hf == 0:
            pl.semaphore_wait(ready, 1)
        spread([(
            lambda d, other: st0.at[hf, c, 1 - my_half if other else my_half, d],
            rt0.at[hf, c, my_half * team + me], T0 + hf, True,
        )], c)

    def collect(hf):
        for c in range(chunks):
            arrive(rt0.at[hf, c], T0 + hf, c)
            lay(c, hf, rt0[hf, c, :team].astype(f32) + rt0[hf, c, team:].astype(f32))
        leave(0, hf)
        enter(1, hf)

    def hand_over(c, hf):
        left, right = project(1, c, hf)
        s1[hf, c, 0] = left
        s1[hf, c, 1] = right
        spread([
            (lambda d, other: s1.at[hf, c, 0, d], rl.at[hf, c, my_half * team + me], L1 + hf, True),
            (lambda d, other: s1.at[hf, c, 1, d], rr.at[hf, c, me], R1 + hf, False),
        ], c)

    def take(c, hf):
        arrive(rl.at[hf, c], L1 + hf, c)
        arrive(rr.at[hf, c], R1 + hf, c)
        unfold([
            (lambda d: rl[hf, c, d], into(ll.at[c, 0], hf)),
            (lambda d: rl[hf, c, team + d], into(ll.at[c, 1], hf)),
            (lambda d: rr[hf, c, d], into(lr.at[c], hf)),
        ])

    def contract(c):
        sums = [
            [
                lax.dot_general(
                    ll[c, h, e], lr[c, e], (((0,), (0,)), ((), ())), preferred_element_type=f32
                )
                for h in range(2)
            ]
            for e in range(each)
        ]

        def piece(hf):
            def pick(e, r, a):
                at = r * first + hf * part + a * depth
                return sums[e][at // LANES][at % LANES:at % LANES + depth]

            def put(d, tile):
                st1[c, d, hf] = tile
            return pick, put

        refold([piece(hf) for hf in range(2)])
        spread([(lambda d, other: st1.at[c, d], rt1.at[c, me], T1, False)], c)

    for load in loading[:2]:
        load.wait()
    for hf in range(2):
        for q in range(depth):
            tile = jnp.concatenate(
                [x_ref[hf * part + a * depth + q] for a in range(fold)], axis=0
            )
            t = hf * span + q * LANES
            xt[:, t:t + LANES] = tile.astype(f32).T
        enter(0, hf)
    loading[2].wait()
    weight_turn(0)
    for c in range(chunks):
        for hf in range(2):
            left, right = project(0, c, hf)
            if hf == 0:
                sa[c, :, 0] = left
            else:
                sb[c] = left
            sa[c, :, 1 + hf] = right
        if c == 0:
            pl.semaphore_wait(barrier, team)
            pl.semaphore_signal(
                ready, inc=1, device_id=device(0, True), device_id_type=pl.DeviceIdType.MESH
            )
        spread([(lambda d, other: sa.at[c, d], ra.at[c, me], HA, False)], c)
    rest_of_setup()
    for c in range(1):
        multiply(c, 0)
    for c in range(chunks):
        spread([(lambda d, other: sb.at[c, d], rb.at[c, me], HB, False)], c)
    for hf in range(2):
        open_gate(0, hf)
    for c in range(1, chunks):
        multiply(c, 0)
    for c in range(chunks):
        multiply(c, 1)
    collect(0)
    for c in range(chunks):
        hand_over(c, 0)
    open_gate(1, 0)
    collect(1)
    for c in range(chunks):
        hand_over(c, 1)
    open_gate(1, 1)
    for c in range(chunks):
        take(c, 0)
    for c in range(chunks):
        take(c, 1)
        contract(c)
    for c in range(chunks):
        arrive(rt1.at[c], T1, c)
        for hf in range(2):
            lay(c, hf, rt1[c, :, hf].astype(f32))
    for hf in range(2):
        leave(1, hf)
    o_ref[...] = xt[...].astype(bf16)

    for c in range(chunks):
        near, both = pl.ds(0, team - 1), pl.ds(0, 2 * team - 1)
        gone(ra.at[c, near], HA, c)
        gone(rb.at[c, near], HB, c)
        for hf in range(2):
            gone(rl.at[hf, c, both], L1 + hf, c)
            gone(rr.at[hf, c, near], R1 + hf, c)
            gone(rt0.at[hf, c, both], T0 + hf, c)
        gone(rt1.at[c, near], T1, c)


def finish(fold, t_ref, o_ref):
    first, second, _ = o_ref.shape
    part = first // 2
    depth = part // fold
    for hf in range(2):
        for q in range(depth):
            t = (hf * depth + q) * LANES
            tile = t_ref[:, t:t + LANES].astype(f32).T.astype(bf16)
            for a in range(fold):
                o_ref[hf * part + a * depth + q] = tile[a * second:(a + 1) * second]


def takes(rows, cols, first, second, channels, hidden):
    if LANES % second or channels != LANES or hidden != LANES or cols % 2 or first % 2:
        return False
    team, fold = rows * (cols // 2), LANES // second
    return (
        cols // 2 == fold and CHUNK % team == 0 and (first // 2) % fold == 0
        and rows * first == cols * second == 2 * LANES
        and first // 2 // fold == 8 and CHUNK // team * 8 == PACK
    )


def solution(mesh):
    rows, cols = mesh.shape["row"], mesh.shape["col"]

    def local(pair_rep, proj_weight, gate_weight, out_weight, in_gain, out_gain):
        first, second, channels = pair_rep.shape
        hidden = out_weight.shape[1]
        args = (pair_rep, proj_weight, gate_weight, out_weight, in_gain, out_gain)
        if not takes(rows, cols, first, second, channels, hidden):
            return plain(*args)
        team = rows * (cols // 2)
        fold = LANES // second
        depth = first // 2 // fold
        chunks = hidden // CHUNK
        each = CHUNK // team
        tile = (each * depth, LANES)
        width = 2 * depth * LANES
        vmem = pl.BlockSpec(memory_space=pltpu.VMEM)
        turned = pl.pallas_call(
            functools.partial(kernel, rows, cols),
            out_shape=pltpu.VMEM((channels, width), bf16),
            in_specs=[pl.BlockSpec(memory_space=pl.ANY)] * 6,
            out_specs=vmem,
            scratch_shapes=[
                *(pltpu.VMEM(arg.shape, arg.dtype) for arg in args),
                pltpu.SemaphoreType.DMA((len(args) + 1,)),
                pltpu.VMEM((channels, width), f32),
                pltpu.VMEM((channels, width), bf16),
                pltpu.VMEM((channels, width), f32),
                pltpu.VMEM((hidden, width), f32),
                pltpu.VMEM((2, chunks, 4 * CHUNK, channels), bf16),
                pltpu.VMEM((2, channels, channels), bf16),
                pltpu.VMEM((2, channels, hidden), bf16),
                pltpu.VMEM((fold * LANES, fold * LANES), bf16),
                pltpu.VMEM((2, 2, CHUNK * depth, LANES), f32),
                pltpu.VMEM((CHUNK * depth, LANES), f32),
                pltpu.VMEM((chunks, team, 3) + tile, bf16),
                pltpu.VMEM((chunks, team) + tile, bf16),
                pltpu.VMEM((2, chunks, 2, team) + tile, bf16),
                pltpu.VMEM((chunks, team, 3) + tile, bf16),
                pltpu.VMEM((chunks, team) + tile, bf16),
                pltpu.VMEM((2, chunks, 2 * team) + tile, bf16),
                pltpu.VMEM((2, chunks, team) + tile, bf16),
                pltpu.VMEM((each, LANES, LANES), bf16),
                pltpu.VMEM((chunks, each, 2 * LANES, LANES), bf16),
                pltpu.VMEM((2, chunks, 2, team) + tile, bf16),
                pltpu.VMEM((2, chunks, 2 * team) + tile, bf16),
                pltpu.VMEM((chunks, 2, each, 2 * LANES, LANES), bf16),
                pltpu.VMEM((chunks, each, 2 * LANES, LANES), bf16),
                pltpu.VMEM((chunks, team, 2) + tile, bf16),
                pltpu.VMEM((chunks, team, 2) + tile, bf16),
                pltpu.SemaphoreType.DMA((18, chunks)),
                pltpu.SemaphoreType.REGULAR,
            ],
            compiler_params=pltpu.CompilerParams(
                collective_id=0, has_side_effects=True, vmem_limit_bytes=62 * 2 ** 20
            ),
        )(*args)
        return pl.pallas_call(
            functools.partial(finish, fold),
            out_shape=jax.ShapeDtypeStruct(pair_rep.shape, bf16),
            in_specs=[vmem],
            out_specs=vmem,
            compiler_params=pltpu.CompilerParams(vmem_limit_bytes=4 * 2 ** 20),
        )(turned)

    return jax.shard_map(
        local,
        mesh=mesh,
        in_specs=(P("row", "col", None), P(), P(), P(), P(), P()),
        out_specs=P("row", "col", None),
        check_vma=False,
    )
```
